32 devices in a mesh: shot: 8 (over z, y), depth: 4 (over x, core).
Axes of the slice: x: 2, y: 2, z: 4, core: 2. Of those that a mesh axis runs over, the one named last changes fastest.
Arguments:
- correlation: float32 [16, 16, 32, 512], P('shot', None, None, 'depth'), may hold values from -6 to 6
- illumination: float32 [16, 16, 32, 512], P('shot', None, None, 'depth'), may hold values from 0.25 to 4
- aperture: int32 [16, 4], P('shot'), may hold values from 0 to 32, as said below
Outputs:
- stack: float32 [16, 32, 512], P('shot', None, 'depth')
The draws below stay inside these ranges and needn't reach their ends.
Inputs may be any that keep to these rules, and one draw needn't show every extreme that they name: For every shot, 0 <= aperture[s,0] < aperture[s,1] <= 16 and 0 <= aperture[s,2] < aperture[s,3] <= 32; each box spans a quarter to a half of the grid along each of the two dimensions.
All inputs are finite; a program needn't handle non-finite values.
Results may differ from the reference program's by a relative error of at most 0.0003.
Values sent between devices are 32-bit elements.
A program may use at most 64 MiB of HBM per device.

```python
import math
import jax
import jax.numpy as jnp
from jax import lax

NY = 32
SHOTS = 16
NX = 16
NZ = 512


def draw_aperture(key, part):
    key_first = jax.random.fold_in(key, 11)
    key_second = jax.random.fold_in(key, 23)
    k_one, k_two = jax.random.split(key_first)
    k_three, k_four = jax.random.split(key_second)
    low_first = jax.random.randint(k_one, (SHOTS,), 0, NX // 2)
    span_first = jax.random.randint(k_two, (SHOTS,), max(NX // 4, 1), NX // 2 + 1)
    low_second = jax.random.randint(k_three, (SHOTS,), 0, NY // 2)
    span_second = jax.random.randint(k_four, (SHOTS,), max(NY // 4, 1), NY // 2 + 1)
    return jnp.stack([low_first, low_first + span_first, low_second, low_second + span_second], axis=1).astype(jnp.int32)


def spiked(values, rng, source, target, blocks, factor):
    owner, partner = [(jnp.arange(values.shape[position]) // (values.shape[position] // blocks)).reshape([-1 if axis == position else 1 for axis in range(values.ndim)]) for position in (source, target)]
    chosen = jax.random.permutation(rng, blocks)[partner]
    strong = (owner == chosen) | (owner == (partner + blocks // 2) % blocks)
    return jnp.where(strong, factor * values, values)


def steps_of(stream_key, dims, pieces, smallest, high):
    def one(dim, blocks):
        draws = jax.random.uniform(jax.random.fold_in(jax.random.fold_in(stream_key, 6), dim), (blocks,), jnp.float32, smallest / len(pieces), high / len(pieces))
        return jnp.repeat(jnp.exp(draws), dims[dim] // blocks).reshape((-1,) + (1,) * (len(dims) - dim - 1))

    gain = one(*pieces[0])
    for cut in pieces[1:]:
        gain = gain * one(*cut)
    return gain


def gaussian_with(stream_key, dims, width, most, pieces, heavy, kind=jnp.bfloat16):
    array = width * jax.random.normal(stream_key, dims, jnp.float32)
    if pieces:
        array = array * steps_of(stream_key, dims, pieces, -0.22, 0.18)
    return jnp.clip(spiked(array, jax.random.fold_in(stream_key, 3), *heavy), -most, most).astype(kind)


def setup_inputs(seed: int = 0) -> dict:
    seeds = jax.random.split(jax.random.key(seed), 4)
    correlation = gaussian_with(seeds[0], (SHOTS, NX, NY, NZ), 1.0, 6.0, ((0, 8), (3, 4)), (0, 1, 8, 2.0), jnp.float32)
    illumination = jnp.clip(jnp.exp(math.log(4.0) - 2.7725887 * jax.random.uniform(seeds[1], (SHOTS, NX, NY, NZ), jnp.float32) ** steps_of(seeds[1], (SHOTS, NX, NY, NZ), ((0, 8), (3, 4)), -0.2, 0.2)), 0.25, 4.0)
    aperture = draw_aperture(jax.random.fold_in(seeds[3], 71), 0)
    return {"correlation": correlation, "illumination": illumination, "aperture": aperture}


def negative_laplacian(field):
    padded = jnp.pad(field, 1)
    beside = padded[2:, 1:-1, 1:-1] + padded[:-2, 1:-1, 1:-1]
    beside = beside + padded[1:-1, 2:, 1:-1] + padded[1:-1, :-2, 1:-1]
    beside = beside + padded[1:-1, 1:-1, 2:] + padded[1:-1, 1:-1, :-2]
    return 6.0 * field - beside

def prepare(correlation, illumination, box):
    first = lax.broadcasted_iota(jnp.int32, (NX, NY, 1), 0)
    second = lax.broadcasted_iota(jnp.int32, (NX, NY, 1), 1)
    inside = (first >= box[0]) & (first < box[1]) & (second >= box[2]) & (second < box[3])
    mask = inside.astype(jnp.float32)
    return negative_laplacian(mask * correlation / (illumination + 0.1))

def reference(correlation, illumination, aperture):
    cells = NX * NY * NZ

    def energy(items):
        filtered = prepare(items[0], items[1], items[2])
        return jnp.sum(filtered * filtered) / cells
    meansq = lax.map(energy, (correlation, illumination, aperture))
    peak = jnp.max(meansq)
    weight = 1.0 / jnp.sqrt(meansq + 0.5 * peak + 1.0)

    def accumulate(total, items):
        filtered = prepare(items[0], items[1], items[2])
        return (total + items[3] * filtered, None)
    stack, unused = lax.scan(accumulate, jnp.zeros((NX, NY, NZ), jnp.float32), (correlation, illumination, aperture, weight))
    return stack / jnp.sqrt(jnp.float32(SHOTS))
```

```python
import functools
import math

import jax
import jax.numpy as jnp
from jax import lax
from jax.experimental import pallas as pl
from jax.experimental.pallas import tpu as pltpu
from jax.sharding import PartitionSpec as P

MESH = pl.DeviceIdType.MESH
LANES = 128
SUBLANES = 8


def kernel(dims, corr_hbm, ill_hbm, box_hbm, out_ref, box, corr, ill, norm, edge_out, edge_in, send, recv, side_out, side_in,
           place_out, place, message, inbox, spread, load_sem, box_sem, ready, edge_send, edge_recv, bulk_send, bulk_recv,
           side_send, side_recv, place_send, place_recv, note_send, note_recv):
    shots, rows, cols, slab, groups, slabs, owned, cells = dims
    half = cols // 2
    tiles = half // SUBLANES
    devices = groups * slabs
    per_pack = LANES // 2
    group = lax.axis_index("shot")
    depth = lax.axis_index("depth")
    place_in_order = group * slabs + depth

    box_copy = pltpu.make_async_copy(box_hbm, box, box_sem)
    box_copy.start()
    loads = []
    for s in range(shots):
        for index, (source, target) in enumerate(((corr_hbm, corr), (ill_hbm, ill))):
            copy = pltpu.make_async_copy(source.at[s], target.at[s], load_sem.at[index, s])
            copy.start()
            loads.append(copy)

    def at(t):
        return {"shot": lax.div(t, slabs), "depth": lax.rem(t, slabs)}

    barrier = pltpu.get_barrier_semaphore()

    def greet(t, carry):
        pl.semaphore_signal(barrier, inc=1, device_id=at(t), device_id_type=MESH)
        return carry

    lax.fori_loop(place_in_order + 1, devices, greet, 0)

    lane = lax.broadcasted_iota(jnp.int32, (SUBLANES, LANES), 1)
    sub = lax.broadcasted_iota(jnp.int32, (SUBLANES, LANES), 0)
    zero = jnp.zeros((SUBLANES, slab), jnp.float32)
    for s in range(shots):
        for r in (0, rows + 1):
            for t in range(tiles + 2):
                norm[s, r, pl.ds(t * SUBLANES, SUBLANES)] = zero
    packs = edge_out.shape[0]

    @pl.when(depth == 0)
    def _():
        for p in range(packs):
            edge_in[0, p] = zero

    @pl.when(depth == slabs - 1)
    def _():
        for p in range(packs):
            edge_in[1, p] = zero

    @pl.when(place_in_order > 0)
    def _():
        pl.semaphore_wait(barrier, place_in_order)

    def answer(i, carry):
        t = place_in_order - 1 - i
        pl.semaphore_signal(ready.at[group], inc=1, device_id=at(t), device_id_type=MESH)
        return carry

    lax.fori_loop(0, place_in_order, answer, 0)

    box_copy.wait()
    lower = []
    upper = []
    start = []
    for s in range(shots):
        first, last = box[s, 2], box[s, 3]
        start.append(jnp.minimum(first, half))
        lower.append([(sub + t * SUBLANES >= first) & (sub + t * SUBLANES < last) for t in range(tiles)])
        upper.append([(sub + t * SUBLANES + half >= first) & (sub + t * SUBLANES + half < last) for t in range(tiles)])
        place_out[pl.ds(s, 1)] = jnp.full((1, LANES), start[s].astype(jnp.float32))
    for copy in loads:
        copy.wait()

    row_index = lax.broadcasted_iota(jnp.int32, (rows, slab), 0)
    energies = []
    for s in range(shots):
        in_rows = (row_index >= box[s, 0]) & (row_index < box[s, 1])
        energy = None
        for side, column in enumerate((start[s], start[s] + half - 1)):
            in_box = (column >= box[s, 2]) & (column < box[s, 3])
            value = jnp.where(in_rows & in_box, corr[s, :, column], 0.0) / (ill[s, :, column] + 0.1)
            side_out[2 * s + side] = 0.0 - value
            in_grid = (start[s] > 0) if side == 0 else (start[s] < cols - half)
            kept = jnp.where(in_grid, value, 0.0)
            kept = kept * kept
            energy = kept if energy is None else energy + kept
        while energy.shape[0] > SUBLANES:
            energy = energy[:energy.shape[0] // 2] + energy[energy.shape[0] // 2:]
        energies.append(energy)

    def lane_of(r, s, t):
        k = (r * shots + s) * tiles + t
        return k // per_pack, 2 * (k % per_pack)

    packed = [zero] * packs
    for r in range(rows):
        for s in range(shots):
            in_row = (r >= box[s, 0]) & (r < box[s, 1])
            parts = []
            for t in range(tiles):
                here = pl.ds(t * SUBLANES, SUBLANES)
                there = pl.ds(t * SUBLANES + half, SUBLANES)
                top = jnp.where(upper[s][t], corr[s, r, there], corr[s, r, here])
                top = jnp.where((lower[s][t] | upper[s][t]) & in_row, top, 0.0)
                value = top / (jnp.where(upper[s][t], ill[s, r, there], ill[s, r, here]) + 0.1)
                parts.append(value)
                p, k = lane_of(r, s, t)
                packed[p] = jnp.where(lane // 2 == k // 2, pltpu.roll(value, k + 1, 1), packed[p])
            for t, value in enumerate([parts[-1]] + parts + [parts[0]]):
                norm[s, r + 1, pl.ds(t * SUBLANES, SUBLANES)] = value
    for p in range(packs):
        edge_out[p] = packed[p]

    def edge_copy(side):
        return pltpu.make_async_remote_copy(
            src_ref=edge_out, dst_ref=edge_in.at[1 - side], send_sem=edge_send.at[side],
            recv_sem=edge_recv.at[1 - side], device_id={"depth": depth + (1 if side else -1)}, device_id_type=MESH)

    @pl.when(depth > 0)
    def _():
        edge_copy(0).start()

    @pl.when(depth < slabs - 1)
    def _():
        pl.semaphore_wait(ready.at[group], slabs - 1 - depth)
        edge_copy(1).start()

    @pl.when(depth > 0)
    def _():
        edge_copy(0).wait_send()
        edge_copy(1).wait_recv()

    @pl.when(depth < slabs - 1)
    def _():
        edge_copy(1).wait_send()
        edge_copy(0).wait_recv()

    no_before = [[sub + t * SUBLANES == lax.rem(start[s], half) for t in range(tiles)] for s in range(shots)]
    no_after = [[sub + t * SUBLANES == lax.rem(start[s] + half - 1, half) for t in range(tiles)] for s in range(shots)]
    halo = [jnp.where(lane % 2 == 0, edge_in[0, p], edge_in[1, p]) for p in range(packs)]
    for r in range(rows):
        owner, i = r // owned, r % owned
        for s in range(shots):
            for t in range(tiles):
                base = SUBLANES + t * SUBLANES
                value = norm[s, r + 1, pl.ds(base, SUBLANES)]
                beside = norm[s, r, pl.ds(base, SUBLANES)] + norm[s, r + 2, pl.ds(base, SUBLANES)]
                beside = beside + jnp.where(no_before[s][t], 0.0, norm[s, r + 1, pl.ds(base - 1, SUBLANES)])
                beside = beside + jnp.where(no_after[s][t], 0.0, norm[s, r + 1, pl.ds(base + 1, SUBLANES)])
                p, k = lane_of(r, s, t)
                near = pltpu.roll(halo[p], LANES - 1 - k, 1)
                left = jnp.where(lane == LANES - 1, near, value)
                right = jnp.where(lane == 0, near, value)
                beside = beside + pltpu.roll(left, 1, 1) + pltpu.roll(right, LANES - 1, 1)
                result = 6.0 * value - beside
                energies[s] = energies[s] + result * result
                send[owner, pl.ds((s * owned + i) * half + t * SUBLANES, SUBLANES)] = result

    def total(value):
        return jnp.sum(jnp.sum(value, axis=0, keepdims=True), axis=1, keepdims=True)

    note = jnp.zeros((1, LANES), jnp.float32)
    gap = LANES // shots
    lane_row = lax.broadcasted_iota(jnp.int32, (1, LANES), 1)
    for s in range(shots):
        note = jnp.where(lane_row // gap == s, total(energies[s]), note)
    message[pl.ds(0, 1)] = note / cells

    slot = depth * groups + group
    own_note = pltpu.make_async_copy(message.at[pl.ds(0, 1)], inbox.at[pl.ds(slot, 1)], note_recv)
    own_note.start()

    def tell(g, d):
        pltpu.make_async_remote_copy(
            src_ref=message.at[pl.ds(0, 1)], dst_ref=inbox.at[pl.ds(slot, 1)], send_sem=note_send, recv_sem=note_recv,
            device_id={"shot": g, "depth": d}, device_id_type=MESH).start()

    def bulk(g, origin):
        return pltpu.make_async_remote_copy(
            src_ref=send.at[g], dst_ref=recv.at[origin], send_sem=bulk_send.at[g], recv_sem=bulk_recv.at[origin],
            device_id={"shot": g}, device_id_type=MESH)

    def side_copy(g, origin):
        return pltpu.make_async_remote_copy(
            src_ref=side_out.at[:, pl.ds(g * owned, owned)], dst_ref=side_in.at[origin], send_sem=side_send.at[g],
            recv_sem=side_recv.at[origin], device_id={"shot": g}, device_id_type=MESH)

    def place_copy(g, origin):
        return pltpu.make_async_remote_copy(
            src_ref=place_out, dst_ref=place.at[origin], send_sem=place_send.at[g], recv_sem=place_recv.at[origin],
            device_id={"shot": g}, device_id_type=MESH)

    for g in range(groups):
        @pl.when(g < group)
        def _():
            for d in range(slabs):
                tell(g, d)
    for d in range(slabs):
        @pl.when(d != depth)
        def _():
            tell(group, d)
    for g in range(groups):
        @pl.when(g < group)
        def _():
            place_copy(g, group).start()
            side_copy(g, group).start()
            bulk(g, group).start()
    for g in range(1, groups):
        @pl.when(g > group)
        def _():
            pl.semaphore_wait(ready.at[g], slabs)
            for d in range(slabs):
                tell(g, d)
            place_copy(g, group).start()
            side_copy(g, group).start()
            bulk(g, group).start()

    recv[group] = send[group]
    side_in[group] = side_out[:, pl.ds(group * owned, owned)]
    place[group] = place_out[...]

    col = [(sub + t * SUBLANES).astype(jnp.float32) for t in range(2 * tiles)]
    for g in range(groups):
        @pl.when(g != group)
        def _():
            place_copy(g, g).wait_recv()
            side_copy(g, g).wait_recv()
            bulk(g, g).wait_recv()

        for s in range(shots):
            first = place[g, pl.ds(s, 1)]
            masks = []
            for t in range(2 * tiles):
                offset = col[t] - first
                masks.append((offset == -1.0, offset == float(half), (offset >= -1.0) & (offset <= float(half))))
            for i in range(owned):
                index = s * owned + i
                low = side_in[g, 2 * s, pl.ds(i, 1)]
                high = side_in[g, 2 * s + 1, pl.ds(i, 1)]
                for t in range(2 * tiles):
                    at_low, at_high, inside = masks[t]
                    value = recv[g, pl.ds(index * half + (t % tiles) * SUBLANES, SUBLANES)]
                    value = jnp.where(at_low, low, jnp.where(at_high, high, value))
                    spread[g, s, i, pl.ds(t * SUBLANES, SUBLANES)] = jnp.where(inside, value, 0.0)

    pltpu.make_async_copy(inbox, inbox, note_recv).wait()
    meansq = inbox[pl.ds(0, groups)]
    for d in range(1, slabs):
        meansq = meansq + inbox[pl.ds(d * groups, groups)]
    peak = jnp.max(meansq, axis=0, keepdims=True)
    turned = peak
    for s in range(1, shots):
        turned = jnp.maximum(turned, pltpu.roll(peak, s * gap, 1))
    weight = (1.0 / math.sqrt(shots * groups)) / jnp.sqrt(meansq + 0.5 * turned + 1.0)
    lane_group = lax.broadcasted_iota(jnp.int32, (groups, LANES), 1) // gap
    sums = [[zero] * (2 * tiles) for i in range(owned)]
    for s in range(shots):
        factor = weight
        for j in range(1, shots):
            factor = jnp.where(lane_group == (s + j) % shots, pltpu.roll(weight, j * gap, 1), factor)
        for g in range(groups):
            for i in range(owned):
                for t in range(2 * tiles):
                    sums[i][t] = sums[i][t] + factor[g:g + 1] * spread[g, s, i, pl.ds(t * SUBLANES, SUBLANES)]
    for i in range(owned):
        for t in range(2 * tiles):
            out_ref[i, pl.ds(t * SUBLANES, SUBLANES)] = sums[i][t]

    pltpu.make_async_copy(inbox.at[pl.ds(0, devices - 1)], inbox.at[pl.ds(0, devices - 1)], note_send).wait()
    for g in range(groups):
        @pl.when(g != group)
        def _():
            place_copy(g, g).wait_send()
            side_copy(g, g).wait_send()
            bulk(g, g).wait_send()


def on_device(correlation, illumination, aperture):
    shots, rows, cols, slab = correlation.shape
    groups = lax.axis_size("shot")
    slabs = lax.axis_size("depth")
    owned = rows // groups
    half = cols // 2
    tiles = half // SUBLANES
    dims = (shots, rows, cols, slab, groups, slabs, owned, rows * cols * slab * slabs)
    packs = -(-rows * shots * tiles // (LANES // 2))
    block = (shots * owned * half, slab)
    f32 = jnp.float32
    dma = pltpu.SemaphoreType.DMA
    return pl.pallas_call(
        functools.partial(kernel, dims),
        out_shape=pltpu.VMEM((owned, cols, slab), f32),
        in_specs=[pl.BlockSpec(memory_space=pl.ANY)] * 3,
        out_specs=pl.BlockSpec(memory_space=pltpu.VMEM),
        scratch_shapes=[
            pltpu.SMEM(aperture.shape, jnp.int32),
            pltpu.VMEM((shots, rows, cols, slab), f32),
            pltpu.VMEM((shots, rows, cols, slab), f32),
            pltpu.VMEM((shots, rows + 2, half + 2 * SUBLANES, slab), f32),
            pltpu.VMEM((packs, SUBLANES, LANES), f32),
            pltpu.VMEM((2, packs, SUBLANES, LANES), f32),
            pltpu.VMEM((groups,) + block, f32),
            pltpu.VMEM((groups,) + block, f32),
            pltpu.VMEM((2 * shots, rows, slab), f32),
            pltpu.VMEM((groups, 2 * shots, owned, slab), f32),
            pltpu.VMEM((shots, LANES), f32),
            pltpu.VMEM((groups, shots, LANES), f32),
            pltpu.VMEM((SUBLANES, LANES), f32),
            pltpu.VMEM((slabs * groups, LANES), f32),
            pltpu.VMEM((groups, shots, owned, cols, slab), f32),
            dma((2, shots)),
            dma,
            pltpu.SemaphoreType.REGULAR((groups,)),
            dma((2,)),
            dma((2,)),
            dma((groups,)),
            dma((groups,)),
            dma((groups,)),
            dma((groups,)),
            dma((groups,)),
            dma((groups,)),
            dma,
            dma,
        ],
        compiler_params=pltpu.CompilerParams(collective_id=0, has_side_effects=True),
    )(correlation, illumination, aperture)


def solution(mesh):
    return jax.shard_map(
        on_device,
        mesh=mesh,
        in_specs=(P("shot", None, None, "depth"), P("shot", None, None, "depth"), P("shot", None)),
        out_specs=P("shot", None, "depth"),
        check_vma=False,
    )
```

```python
import functools
import math

import jax
import jax.numpy as jnp
from jax import lax
from jax.experimental import pallas as pl
from jax.experimental.pallas import tpu as pltpu
from jax.sharding import PartitionSpec as P

MESH = pl.DeviceIdType.MESH
LANES = 128
SUBLANES = 8
EARLY = 1


def kernel(dims, corr_hbm, ill_hbm, box_hbm, out_ref, box, raw, norm, centre, edge_out, edge_in, halo_out, halo_in, halves, send, recv, message, inbox, spread,
           load_sem, box_sem, ready, passed, edge_send, edge_recv, bulk_send, bulk_recv, halo_send, halo_recv, note_send, note_recv):
    shots, rows, cols, slab, groups, slabs, owned, cells = dims
    half = cols // 2
    tiles = half // SUBLANES
    devices = groups * slabs
    per_pack = LANES // 2
    per_owner = owned * shots * tiles
    group = lax.axis_index("shot")
    depth = lax.axis_index("depth")
    border = shots * owned * half
    placed = border + 2 * shots * owned
    corr, ill = raw.at[0], raw.at[1]

    box_copy = pltpu.make_async_copy(box_hbm, box, box_sem)
    box_copy.start()
    for s in range(shots):
        for source, target in ((corr_hbm, corr), (ill_hbm, ill)):
            pltpu.make_async_copy(source.at[s], target.at[s], load_sem).start()

    def signal(semaphore, **device):
        pl.semaphore_signal(semaphore, inc=1, device_id=device, device_id_type=MESH)

    def each(low, high, action):
        lax.fori_loop(low, high, lambda t, carry: (action(t), carry)[1], 0)

    barrier = pltpu.get_barrier_semaphore()
    each(1, slabs, lambda d: signal(barrier, depth=lax.rem(depth + d, slabs)))
    each(group + 1, groups, lambda g: signal(barrier, shot=g))

    lane = lax.broadcasted_iota(jnp.int32, (SUBLANES, LANES), 1)
    sub = lax.broadcasted_iota(jnp.int32, (SUBLANES, LANES), 0)
    zero = jnp.zeros((SUBLANES, slab), jnp.float32)
    for s in range(shots):
        for r in (0, rows + 1):
            for t in range(tiles + 2):
                norm[s, r, pl.ds(t * SUBLANES, SUBLANES)] = zero
    packs = edge_out.shape[0]

    @pl.when(depth == 0)
    def _():
        for p in range(packs):
            edge_in[0, p] = zero

    @pl.when(depth == slabs - 1)
    def _():
        for p in range(packs):
            edge_in[1, p] = zero

    box_copy.wait()
    lower = []
    upper = []
    start = []
    for s in range(shots):
        first, last = box[s, 2], box[s, 3]
        start.append(jnp.minimum(first, half))
        lower.append([(sub + t * SUBLANES >= first) & (sub + t * SUBLANES < last) for t in range(tiles)])
        upper.append([(sub + t * SUBLANES + half >= first) & (sub + t * SUBLANES + half < last) for t in range(tiles)])
    pltpu.make_async_copy(raw, raw, load_sem).wait()

    row_index = lax.broadcasted_iota(jnp.int32, (rows, slab), 0)
    energies = []
    for s in range(shots):
        in_rows = (row_index >= box[s, 0]) & (row_index < box[s, 1])
        energy = None
        for side, column in enumerate((start[s], start[s] + half - 1)):
            in_box = (column >= box[s, 2]) & (column < box[s, 3])
            value = jnp.where(in_rows & in_box, corr[s, :, column], 0.0) / (ill[s, :, column] + 0.1)
            for owner in range(groups):
                send[owner, pl.ds(border + (2 * s + side) * owned, owned)] = 0.0 - value[owner * owned:(owner + 1) * owned]
            in_grid = (start[s] > 0) if side == 0 else (start[s] < cols - half)
            kept = jnp.where(in_grid, value, 0.0)
            kept = kept * kept
            energy = kept if energy is None else energy + kept
        while energy.shape[0] > SUBLANES:
            energy = energy[:energy.shape[0] // 2] + energy[energy.shape[0] // 2:]
        energies.append(energy)
        for owner in range(groups):
            send[owner, pl.ds(placed + s, 1)] = jnp.full((1, LANES), start[s].astype(jnp.float32))

    def lane_of(r, s, t):
        k = (r * shots + s) * tiles + t
        return k // per_pack, 2 * (k % per_pack)

    packed = [zero] * packs
    for r in range(rows):
        for s in range(shots):
            in_row = (r >= box[s, 0]) & (r < box[s, 1])
            parts = []
            for t in range(tiles):
                here = pl.ds(t * SUBLANES, SUBLANES)
                there = pl.ds(t * SUBLANES + half, SUBLANES)
                top = jnp.where(upper[s][t], corr[s, r, there], corr[s, r, here])
                top = jnp.where((lower[s][t] | upper[s][t]) & in_row, top, 0.0)
                value = top / (jnp.where(upper[s][t], ill[s, r, there], ill[s, r, here]) + 0.1)
                parts.append(value)
                p, k = lane_of(r, s, t)
                packed[p] = jnp.where(lane // 2 == k // 2, pltpu.roll(value, k + 1, 1), packed[p])
                beside = jnp.where(lane > 0, pltpu.roll(value, 1, 1), 0.0)
                beside = beside + jnp.where(lane < LANES - 1, pltpu.roll(value, LANES - 1, 1), 0.0)
                centre[s, r, pl.ds(t * SUBLANES, SUBLANES)] = 6.0 * value - beside
            for t, value in enumerate([parts[-1]] + parts + [parts[0]]):
                norm[s, r + 1, pl.ds(t * SUBLANES, SUBLANES)] = value
    for p in range(packs):
        edge_out[p] = packed[p]

    def edge_copy(side):
        return pltpu.make_async_remote_copy(
            src_ref=edge_out, dst_ref=edge_in.at[1 - side], send_sem=edge_send.at[side],
            recv_sem=edge_recv.at[1 - side], device_id={"depth": depth + (1 if side else -1)}, device_id_type=MESH)

    pl.semaphore_wait(barrier, group + slabs - 1)

    @pl.when(depth > 0)
    def _():
        edge_copy(0).start()

    @pl.when(depth < slabs - 1)
    def _():
        edge_copy(1).start()

    each(0, group, lambda g: signal(ready.at[group], shot=g))
    each(1, slabs, lambda d: signal(passed, depth=lax.rem(depth + d, slabs)))

    no_before = [[sub + t * SUBLANES == lax.rem(start[s], half) for t in range(tiles)] for s in range(shots)]
    no_after = [[sub + t * SUBLANES == lax.rem(start[s] + half - 1, half) for t in range(tiles)] for s in range(shots)]
    packed = [zero] * packs
    for r in range(rows):
        owner, i = r // owned, r % owned
        for s in range(shots):
            for t in range(tiles):
                base = SUBLANES + t * SUBLANES
                beside = norm[s, r, pl.ds(base, SUBLANES)] + norm[s, r + 2, pl.ds(base, SUBLANES)]
                beside = beside + jnp.where(no_before[s][t], 0.0, norm[s, r + 1, pl.ds(base - 1, SUBLANES)])
                beside = beside + jnp.where(no_after[s][t], 0.0, norm[s, r + 1, pl.ds(base + 1, SUBLANES)])
                p, k = lane_of(r, s, t)
                result = centre[s, r, pl.ds(t * SUBLANES, SUBLANES)] - beside
                energies[s] = energies[s] + result * result
                packed[p] = jnp.where(lane // 2 == k // 2, pltpu.roll(result, k + 1, 1), packed[p])
                send[owner, pl.ds((s * owned + i) * half + t * SUBLANES, SUBLANES)] = result

    def bulk(g, origin):
        return pltpu.make_async_remote_copy(
            src_ref=send.at[g], dst_ref=recv.at[origin], send_sem=bulk_send, recv_sem=bulk_recv.at[origin],
            device_id={"shot": g}, device_id_type=MESH)

    def halo_copy(g):
        return pltpu.make_async_remote_copy(
            src_ref=halo_out.at[g * per_owner // per_pack], dst_ref=halo_in.at[group], send_sem=halo_send,
            recv_sem=halo_recv, device_id={"shot": g}, device_id_type=MESH)

    for g in range(min(EARLY, groups)):
        @pl.when(g < group)
        def _():
            bulk(g, group).start()

    @pl.when(depth > 0)
    def _():
        edge_copy(0).wait_send()
        edge_copy(1).wait_recv()

    @pl.when(depth < slabs - 1)
    def _():
        edge_copy(1).wait_send()
        edge_copy(0).wait_recv()

    lane_shot = lax.rem(lane // (2 * tiles), shots)
    for p in range(packs):
        halo = jnp.where(lane % 2 == 0, pltpu.roll(edge_in[1, p], LANES - 1, 1), pltpu.roll(edge_in[0, p], 1, 1))
        halo_out[p] = halo
        change = halo * (halo - 2.0 * packed[p])
        for s in range(shots):
            energies[s] = energies[s] + jnp.where(lane_shot == s, change, 0.0)

    def total(value):
        return jnp.sum(jnp.sum(value, axis=0, keepdims=True), axis=1, keepdims=True)

    note = jnp.zeros((1, LANES), jnp.float32)
    gap = LANES // shots
    lane_row = lax.broadcasted_iota(jnp.int32, (1, LANES), 1)
    for s in range(shots):
        note = jnp.where(lane_row // gap == s, total(energies[s]), note)
    message[pl.ds(0, 1)] = note / cells

    slot = depth * groups + group
    own_note = pltpu.make_async_copy(message.at[pl.ds(0, 1)], inbox.at[pl.ds(slot, 1)], note_recv)
    own_note.start()

    def tell(g, d):
        pltpu.make_async_remote_copy(
            src_ref=message.at[pl.ds(0, 1)], dst_ref=inbox.at[pl.ds(slot, 1)], send_sem=note_send, recv_sem=note_recv,
            device_id={"shot": g, "depth": d}, device_id_type=MESH).start()

    pl.semaphore_wait(passed, slabs - 1)
    for g in range(groups):
        @pl.when(g < group)
        def _():
            for d in range(slabs):
                tell(g, d)
    for d in range(slabs):
        @pl.when(d != depth)
        def _():
            tell(group, d)
    for g in range(groups):
        @pl.when(g < group)
        def _():
            halo_copy(g).start()
    for g in range(EARLY, groups):
        @pl.when(g < group)
        def _():
            bulk(g, group).start()
    for g in range(1, groups):
        @pl.when(g > group)
        def _():
            pl.semaphore_wait(ready.at[g], 1)
            bulk(g, group).start()
            halo_copy(g).start()
            for d in range(slabs):
                tell(g, d)

    recv[group] = send[group]
    halo_in[group] = halo_out[lax.div(group * per_owner, per_pack)]

    col = [(sub + t * SUBLANES).astype(jnp.float32) for t in range(2 * tiles)]
    for g in range(groups):
        @pl.when(g != group)
        def _():
            bulk(g, g).wait_recv()

        for s in range(shots):
            first = recv[g, pl.ds(placed + s, 1)]
            masks = []
            for t in range(2 * tiles):
                offset = col[t] - first
                masks.append((offset == -1.0, offset == float(half), (offset >= -1.0) & (offset <= float(half))))
            for i in range(owned):
                index = s * owned + i
                low = recv[g, pl.ds(border + 2 * s * owned + i, 1)]
                high = recv[g, pl.ds(border + (2 * s + 1) * owned + i, 1)]
                for t in range(2 * tiles):
                    at_low, at_high, inside = masks[t]
                    value = recv[g, pl.ds(index * half + (t % tiles) * SUBLANES, SUBLANES)]
                    value = jnp.where(at_low, low, jnp.where(at_high, high, value))
                    spread[g, s, i, pl.ds(t * SUBLANES, SUBLANES)] = jnp.where(inside, value, 0.0)

    arrived = halo_in.at[pl.ds(0, groups - 1)]
    pltpu.make_async_copy(arrived, arrived, halo_recv).wait()
    fold_col = (lax.rem(lane // 2, tiles) * SUBLANES + sub).astype(jnp.float32)
    for g in range(groups):
        first = recv[g, pl.ds(placed, 1)]
        for s in range(1, shots):
            first = jnp.where(lane_shot == s, recv[g, pl.ds(placed + s, 1)], first)
        halo = halo_in[g]
        halves[g, 0] = jnp.where(fold_col >= first, halo, 0.0)
        halves[g, 1] = jnp.where(fold_col >= first, 0.0, halo)

    pltpu.make_async_copy(inbox, inbox, note_recv).wait()
    meansq = inbox[pl.ds(0, groups)]
    for d in range(1, slabs):
        meansq = meansq + inbox[pl.ds(d * groups, groups)]
    lane_group = lax.broadcasted_iota(jnp.int32, (groups, LANES), 1) // gap
    turned = [meansq] + [pltpu.roll(meansq, j * gap, 1) for j in range(1, shots)]
    by_shot = []
    for s in range(shots):
        value = meansq
        for j in range(1, shots):
            value = jnp.where(lane_group == (s + j) % shots, turned[j], value)
        by_shot.append(value)
    peak = by_shot[0]
    for s in range(1, shots):
        peak = jnp.maximum(peak, by_shot[s])
    peak = 0.5 * jnp.max(peak, axis=0, keepdims=True) + 1.0
    factors = [(1.0 / math.sqrt(shots * groups)) / jnp.sqrt(by_shot[s] + peak) for s in range(shots)]
    factor = factors[0]
    lane_row_shot = lax.rem(lax.broadcasted_iota(jnp.int32, (groups, LANES), 1) // (2 * tiles), shots)
    for s in range(1, shots):
        factor = jnp.where(lane_row_shot == s, factors[s], factor)
    sums = [[zero] * (2 * tiles) for i in range(owned)]
    for h in range(2):
        halo = zero
        for g in range(groups):
            halo = halo + factor[g:g + 1] * halves[g, h]
        origin = 2 * lax.rem(group * per_owner, per_pack) + 1
        for i in range(owned):
            for t in range(tiles):
                value = zero
                for s in range(shots):
                    place = origin + 2 * ((i * shots + s) * tiles + t)
                    value = value + pltpu.roll(halo, 2 * LANES - place, 1)
                ends = (lane == 0) | (lane == LANES - 1)
                sums[i][h * tiles + t] = jnp.where(ends, 0.0 - value, 0.0)
    for s in range(shots):
        for g in range(groups):
            for i in range(owned):
                for t in range(2 * tiles):
                    sums[i][t] = sums[i][t] + factors[s][g:g + 1] * spread[g, s, i, pl.ds(t * SUBLANES, SUBLANES)]
    for i in range(owned):
        for t in range(2 * tiles):
            out_ref[i, pl.ds(t * SUBLANES, SUBLANES)] = sums[i][t]

    pltpu.make_async_copy(inbox.at[pl.ds(0, devices - 1)], inbox.at[pl.ds(0, devices - 1)], note_send).wait()
    pltpu.make_async_copy(arrived, arrived, halo_send).wait()
    others = send.at[pl.ds(0, groups - 1)]
    pltpu.make_async_copy(others, others, bulk_send).wait()


def on_device(correlation, illumination, aperture):
    shots, rows, cols, slab = correlation.shape
    groups = lax.axis_size("shot")
    slabs = lax.axis_size("depth")
    owned = rows // groups
    half = cols // 2
    tiles = half // SUBLANES
    dims = (shots, rows, cols, slab, groups, slabs, owned, rows * cols * slab * slabs)
    packs = -(-rows * shots * tiles // (LANES // 2))
    block = (shots * owned * (half + 2) + shots, slab)
    f32 = jnp.float32
    dma = pltpu.SemaphoreType.DMA
    regular = pltpu.SemaphoreType.REGULAR
    return pl.pallas_call(
        functools.partial(kernel, dims),
        out_shape=pltpu.VMEM((owned, cols, slab), f32),
        in_specs=[pl.BlockSpec(memory_space=pl.ANY)] * 3,
        out_specs=pl.BlockSpec(memory_space=pltpu.VMEM),
        scratch_shapes=[
            pltpu.SMEM(aperture.shape, jnp.int32),
            pltpu.VMEM((2, shots, rows, cols, slab), f32),
            pltpu.VMEM((shots, rows + 2, half + 2 * SUBLANES, slab), f32),
            pltpu.VMEM((shots, rows, half, slab), f32),
            pltpu.VMEM((packs, SUBLANES, LANES), f32),
            pltpu.VMEM((2, packs, SUBLANES, LANES), f32),
            pltpu.VMEM((packs, SUBLANES, LANES), f32),
            pltpu.VMEM((groups, SUBLANES, LANES), f32),
            pltpu.VMEM((groups, 2, SUBLANES, LANES), f32),
            pltpu.VMEM((groups,) + block, f32),
            pltpu.VMEM((groups,) + block, f32),
            pltpu.VMEM((SUBLANES, LANES), f32),
            pltpu.VMEM((slabs * groups, LANES), f32),
            pltpu.VMEM((groups, shots, owned, cols, slab), f32),
            dma,
            dma,
            regular((groups,)),
            regular,
            dma((2,)),
            dma((2,)),
            dma,
            dma((groups,)),
            dma,
            dma,
            dma,
            dma,
        ],
        compiler_params=pltpu.CompilerParams(collective_id=0, has_side_effects=True),
    )(correlation, illumination, aperture)


def solution(mesh):
    return jax.shard_map(
        on_device,
        mesh=mesh,
        in_specs=(P("shot", None, None, "depth"), P("shot", None, None, "depth"), P("shot", None)),
        out_specs=P("shot", None, "depth"),
        check_vma=False,
    )
```

```python
import functools
import math

import jax
import jax.numpy as jnp
from jax import lax
from jax.experimental import pallas as pl
from jax.experimental.pallas import tpu as pltpu
from jax.sharding import PartitionSpec as P

MESH = pl.DeviceIdType.MESH
LANES = 128
SUBLANES = 8
EARLY = 1


def kernel(dims, corr_hbm, ill_hbm, box_hbm, out_ref, box, raw, norm, centre, edge_out, edge_in, halo_out, halo_in, halves, send, recv, message, inbox, spread,
           load_sem, box_sem, ready, passed, edge_send, edge_recv, bulk_send, bulk_recv, halo_send, halo_recv, note_send, note_recv):
    shots, rows, cols, slab, groups, slabs, owned, cells = dims
    half = cols // 2
    tiles = half // SUBLANES
    devices = groups * slabs
    per_pack = LANES // 2
    per_owner = owned * shots * tiles
    group = lax.axis_index("shot")
    depth = lax.axis_index("depth")
    border = shots * owned * half
    placed = border + 2 * shots * owned
    corr, ill = raw.at[0], raw.at[1]

    box_copy = pltpu.make_async_copy(box_hbm, box, box_sem)
    box_copy.start()
    for s in range(shots):
        for source, target in ((corr_hbm, corr), (ill_hbm, ill)):
            pltpu.make_async_copy(source.at[s], target.at[s], load_sem).start()

    def signal(semaphore, **device):
        pl.semaphore_signal(semaphore, inc=1, device_id=device, device_id_type=MESH)

    def each(low, high, action):
        lax.fori_loop(low, high, lambda t, carry: (action(t), carry)[1], 0)

    barrier = pltpu.get_barrier_semaphore()
    each(1, slabs, lambda d: signal(barrier, depth=lax.rem(depth + d, slabs)))
    each(group + 1, groups, lambda g: signal(barrier, shot=g))

    lane = lax.broadcasted_iota(jnp.int32, (SUBLANES, LANES), 1)
    sub = lax.broadcasted_iota(jnp.int32, (SUBLANES, LANES), 0)
    zero = jnp.zeros((SUBLANES, slab), jnp.float32)
    for s in range(shots):
        for r in (0, rows + 1):
            for t in range(tiles + 2):
                norm[s, r, pl.ds(t * SUBLANES, SUBLANES)] = zero
    packs = edge_out.shape[0]

    @pl.when(depth == 0)
    def _():
        for p in range(packs):
            edge_in[0, p] = zero

    @pl.when(depth == slabs - 1)
    def _():
        for p in range(packs):
            edge_in[1, p] = zero

    box_copy.wait()
    lower = []
    upper = []
    start = []
    for s in range(shots):
        first, last = box[s, 2], box[s, 3]
        start.append(jnp.minimum(first, half))
        lower.append([(sub + t * SUBLANES >= first) & (sub + t * SUBLANES < last) for t in range(tiles)])
        upper.append([(sub + t * SUBLANES + half >= first) & (sub + t * SUBLANES + half < last) for t in range(tiles)])
    pltpu.make_async_copy(raw, raw, load_sem).wait()

    row_index = lax.broadcasted_iota(jnp.int32, (rows, slab), 0)
    energies = []
    for s in range(shots):
        in_rows = (row_index >= box[s, 0]) & (row_index < box[s, 1])
        energy = None
        for side, column in enumerate((start[s], start[s] + half - 1)):
            in_box = (column >= box[s, 2]) & (column < box[s, 3])
            value = jnp.where(in_rows & in_box, corr[s, :, column], 0.0) / (ill[s, :, column] + 0.1)
            for owner in range(groups):
                send[owner, pl.ds(border + (2 * s + side) * owned, owned)] = 0.0 - value[owner * owned:(owner + 1) * owned]
            in_grid = (start[s] > 0) if side == 0 else (start[s] < cols - half)
            kept = jnp.where(in_grid, value, 0.0)
            kept = kept * kept
            energy = kept if energy is None else energy + kept
        while energy.shape[0] > SUBLANES:
            energy = energy[:energy.shape[0] // 2] + energy[energy.shape[0] // 2:]
        energies.append(energy)
        for owner in range(groups):
            send[owner, pl.ds(placed + s, 1)] = jnp.full((1, LANES), start[s].astype(jnp.float32))

    def lane_of(r, s, t):
        k = (r * shots + s) * tiles + t
        return k // per_pack, 2 * (k % per_pack)

    packed = [zero] * packs
    for r in range(rows):
        for s in range(shots):
            in_row = (r >= box[s, 0]) & (r < box[s, 1])
            parts = []
            for t in range(tiles):
                here = pl.ds(t * SUBLANES, SUBLANES)
                there = pl.ds(t * SUBLANES + half, SUBLANES)
                top = jnp.where(upper[s][t], corr[s, r, there], corr[s, r, here])
                top = jnp.where((lower[s][t] | upper[s][t]) & in_row, top, 0.0)
                value = top / (jnp.where(upper[s][t], ill[s, r, there], ill[s, r, here]) + 0.1)
                parts.append(value)
                p, k = lane_of(r, s, t)
                packed[p] = jnp.where(lane // 2 == k // 2, pltpu.roll(value, k + 1, 1), packed[p])
                beside = jnp.where(lane > 0, pltpu.roll(value, 1, 1), 0.0)
                beside = beside + jnp.where(lane < LANES - 1, pltpu.roll(value, LANES - 1, 1), 0.0)
                centre[s, r, pl.ds(t * SUBLANES, SUBLANES)] = 6.0 * value - beside
            for t, value in enumerate([parts[-1]] + parts + [parts[0]]):
                norm[s, r + 1, pl.ds(t * SUBLANES, SUBLANES)] = value
    for p in range(packs):
        edge_out[p] = packed[p]

    def edge_copy(side):
        return pltpu.make_async_remote_copy(
            src_ref=edge_out, dst_ref=edge_in.at[1 - side], send_sem=edge_send.at[side],
            recv_sem=edge_recv.at[1 - side], device_id={"depth": depth + (1 if side else -1)}, device_id_type=MESH)

    pl.semaphore_wait(barrier, group + slabs - 1)

    @pl.when(depth > 0)
    def _():
        edge_copy(0).start()

    @pl.when(depth < slabs - 1)
    def _():
        edge_copy(1).start()

    each(0, group, lambda g: signal(ready.at[group], shot=g))
    each(1, slabs, lambda d: signal(passed, depth=lax.rem(depth + d, slabs)))

    no_before = [[sub + t * SUBLANES == lax.rem(start[s], half) for t in range(tiles)] for s in range(shots)]
    no_after = [[sub + t * SUBLANES == lax.rem(start[s] + half - 1, half) for t in range(tiles)] for s in range(shots)]
    packed = [zero] * packs
    for r in range(rows):
        owner, i = r // owned, r % owned
        for s in range(shots):
            for t in range(tiles):
                base = SUBLANES + t * SUBLANES
                beside = norm[s, r, pl.ds(base, SUBLANES)] + norm[s, r + 2, pl.ds(base, SUBLANES)]
                beside = beside + jnp.where(no_before[s][t], 0.0, norm[s, r + 1, pl.ds(base - 1, SUBLANES)])
                beside = beside + jnp.where(no_after[s][t], 0.0, norm[s, r + 1, pl.ds(base + 1, SUBLANES)])
                p, k = lane_of(r, s, t)
                result = centre[s, r, pl.ds(t * SUBLANES, SUBLANES)] - beside
                energies[s] = energies[s] + result * result
                packed[p] = jnp.where(lane // 2 == k // 2, pltpu.roll(result, k + 1, 1), packed[p])
                send[owner, pl.ds((s * owned + i) * half + t * SUBLANES, SUBLANES)] = result

    def bulk(g, origin):
        return pltpu.make_async_remote_copy(
            src_ref=send.at[g], dst_ref=recv.at[origin], send_sem=bulk_send, recv_sem=bulk_recv.at[origin],
            device_id={"shot": g}, device_id_type=MESH)

    def halo_copy(g):
        return pltpu.make_async_remote_copy(
            src_ref=halo_out.at[g * per_owner // per_pack], dst_ref=halo_in.at[group], send_sem=halo_send.at[g],
            recv_sem=halo_recv, device_id={"shot": g}, device_id_type=MESH)

    early = min(EARLY, groups)
    for g in range(early):
        @pl.when(g < group)
        def _():
            bulk(g, group).start()

    @pl.when(depth > 0)
    def _():
        edge_copy(0).wait_send()
        edge_copy(1).wait_recv()

    @pl.when(depth < slabs - 1)
    def _():
        edge_copy(1).wait_send()
        edge_copy(0).wait_recv()

    lane_shot = lax.rem(lane // (2 * tiles), shots)
    halos = []
    for p in range(packs):
        halo = jnp.where(lane % 2 == 0, pltpu.roll(edge_in[1, p], LANES - 1, 1), pltpu.roll(edge_in[0, p], 1, 1))
        halo_out[p] = halo
        halos.append(halo)
        change = halo * (halo - 2.0 * packed[p])
        for s in range(shots):
            energies[s] = energies[s] + jnp.where(lane_shot == s, change, 0.0)

    def total(value):
        return jnp.sum(jnp.sum(value, axis=0, keepdims=True), axis=1, keepdims=True)

    note = jnp.zeros((1, LANES), jnp.float32)
    gap = LANES // shots
    lane_row = lax.broadcasted_iota(jnp.int32, (1, LANES), 1)
    for s in range(shots):
        note = jnp.where(lane_row // gap == s, total(energies[s]), note)
    message[pl.ds(0, 1)] = note / cells

    slot = depth * groups + group
    own_note = pltpu.make_async_copy(message.at[pl.ds(0, 1)], inbox.at[pl.ds(slot, 1)], note_recv)
    own_note.start()

    def tell(g, d):
        pltpu.make_async_remote_copy(
            src_ref=message.at[pl.ds(0, 1)], dst_ref=inbox.at[pl.ds(slot, 1)], send_sem=note_send, recv_sem=note_recv,
            device_id={"shot": g, "depth": d}, device_id_type=MESH).start()

    pl.semaphore_wait(passed, slabs - 1)
    for g in range(groups):
        @pl.when(g < group)
        def _():
            for d in range(slabs):
                tell(g, d)
    for d in range(slabs):
        @pl.when(d != depth)
        def _():
            tell(group, d)
    for g in range(early):
        @pl.when(g < group)
        def _():
            halo_copy(g).start()
    ends = (lane == 0) | (lane == LANES - 1)
    for owner in range(early, groups):
        for i in range(owned):
            for s in range(shots):
                for t in range(tiles):
                    p, k = lane_of(owner * owned + i, s, t)
                    here = pl.ds((s * owned + i) * half + t * SUBLANES, SUBLANES)
                    moved = pltpu.roll(halos[p], LANES - 1 - k, 1)
                    send[owner, here] = send[owner, here] - jnp.where(ends, moved, 0.0)
    for g in range(early, groups):
        @pl.when(g < group)
        def _():
            bulk(g, group).start()
    for g in sorted(range(1, groups), key=lambda g: (g % 2, g) if 2 * g >= groups else (0, 0)):
        @pl.when(g > group)
        def _():
            pl.semaphore_wait(ready.at[g], 1)
            bulk(g, group).start()
            for d in range(slabs):
                tell(g, d)

    recv[group] = send[group]

    col = [(sub + t * SUBLANES).astype(jnp.float32) for t in range(2 * tiles)]
    for g in range(groups):
        @pl.when(g != group)
        def _():
            bulk(g, g).wait_recv()

        for s in range(shots):
            first = recv[g, pl.ds(placed + s, 1)]
            masks = []
            for t in range(2 * tiles):
                offset = col[t] - first
                masks.append((offset == -1.0, offset == float(half), (offset >= -1.0) & (offset <= float(half))))
            for i in range(owned):
                index = s * owned + i
                low = recv[g, pl.ds(border + 2 * s * owned + i, 1)]
                high = recv[g, pl.ds(border + (2 * s + 1) * owned + i, 1)]
                for t in range(2 * tiles):
                    at_low, at_high, inside = masks[t]
                    value = recv[g, pl.ds(index * half + (t % tiles) * SUBLANES, SUBLANES)]
                    value = jnp.where(at_low, low, jnp.where(at_high, high, value))
                    spread[g, s, i, pl.ds(t * SUBLANES, SUBLANES)] = jnp.where(inside, value, 0.0)

    arrived = halo_in.at[pl.ds(0, groups - 1)]

    @pl.when(group < early)
    def _():
        halo_in[group] = halo_out[lax.div(group * per_owner, per_pack)]
        pltpu.make_async_copy(arrived, arrived, halo_recv).wait()
        fold_col = (lax.rem(lane // 2, tiles) * SUBLANES + sub).astype(jnp.float32)
        for g in range(groups):
            first = recv[g, pl.ds(placed, 1)]
            for s in range(1, shots):
                first = jnp.where(lane_shot == s, recv[g, pl.ds(placed + s, 1)], first)
            halo = halo_in[g]
            halves[g, 0] = jnp.where(fold_col >= first, halo, 0.0)
            halves[g, 1] = jnp.where(fold_col >= first, 0.0, halo)

    pltpu.make_async_copy(inbox, inbox, note_recv).wait()
    meansq = inbox[pl.ds(0, groups)]
    for d in range(1, slabs):
        meansq = meansq + inbox[pl.ds(d * groups, groups)]
    lane_group = lax.broadcasted_iota(jnp.int32, (groups, LANES), 1) // gap
    turned = [meansq] + [pltpu.roll(meansq, j * gap, 1) for j in range(1, shots)]
    by_shot = []
    for s in range(shots):
        value = meansq
        for j in range(1, shots):
            value = jnp.where(lane_group == (s + j) % shots, turned[j], value)
        by_shot.append(value)
    peak = by_shot[0]
    for s in range(1, shots):
        peak = jnp.maximum(peak, by_shot[s])
    peak = 0.5 * jnp.max(peak, axis=0, keepdims=True) + 1.0
    factors = [(1.0 / math.sqrt(shots * groups)) / jnp.sqrt(by_shot[s] + peak) for s in range(shots)]
    for i in range(owned):
        for t in range(2 * tiles):
            total_t = None
            for s in range(shots):
                part = factors[s][0:1] * spread[0, s, i, pl.ds(t * SUBLANES, SUBLANES)]
                for g in range(1, groups):
                    part = part + factors[s][g:g + 1] * spread[g, s, i, pl.ds(t * SUBLANES, SUBLANES)]
                total_t = part if total_t is None else total_t + part
            out_ref[i, pl.ds(t * SUBLANES, SUBLANES)] = total_t

    @pl.when(group < early)
    def _():
        factor = factors[0]
        lane_row_shot = lax.rem(lax.broadcasted_iota(jnp.int32, (groups, LANES), 1) // (2 * tiles), shots)
        for s in range(1, shots):
            factor = jnp.where(lane_row_shot == s, factors[s], factor)
        origin = 2 * lax.rem(group * per_owner, per_pack) + 1
        for h in range(2):
            halo = factor[0:1] * halves[0, h]
            for g in range(1, groups):
                halo = halo + factor[g:g + 1] * halves[g, h]
            for i in range(owned):
                for t in range(tiles):
                    value = None
                    for s in range(shots):
                        shift = 2 * LANES - origin - 2 * ((i * shots + s) * tiles + t)
                        moved = pltpu.roll(halo, shift, 1)
                        value = moved if value is None else value + moved
                    here = pl.ds((h * tiles + t) * SUBLANES, SUBLANES)
                    out_ref[i, here] = out_ref[i, here] - jnp.where(ends, value, 0.0)

    pltpu.make_async_copy(inbox.at[pl.ds(0, devices - 1)], inbox.at[pl.ds(0, devices - 1)], note_send).wait()
    for g in range(early):
        @pl.when(g < group)
        def _():
            halo_copy(g).wait_send()
    others = send.at[pl.ds(0, groups - 1)]
    pltpu.make_async_copy(others, others, bulk_send).wait()


def on_device(correlation, illumination, aperture):
    shots, rows, cols, slab = correlation.shape
    groups = lax.axis_size("shot")
    slabs = lax.axis_size("depth")
    owned = rows // groups
    half = cols // 2
    tiles = half // SUBLANES
    dims = (shots, rows, cols, slab, groups, slabs, owned, rows * cols * slab * slabs)
    packs = -(-rows * shots * tiles // (LANES // 2))
    block = (shots * owned * (half + 2) + shots, slab)
    f32 = jnp.float32
    dma = pltpu.SemaphoreType.DMA
    regular = pltpu.SemaphoreType.REGULAR
    return pl.pallas_call(
        functools.partial(kernel, dims),
        out_shape=pltpu.VMEM((owned, cols, slab), f32),
        in_specs=[pl.BlockSpec(memory_space=pl.ANY)] * 3,
        out_specs=pl.BlockSpec(memory_space=pltpu.VMEM),
        scratch_shapes=[
            pltpu.SMEM(aperture.shape, jnp.int32),
            pltpu.VMEM((2, shots, rows, cols, slab), f32),
            pltpu.VMEM((shots, rows + 2, half + 2 * SUBLANES, slab), f32),
            pltpu.VMEM((shots, rows, half, slab), f32),
            pltpu.VMEM((packs, SUBLANES, LANES), f32),
            pltpu.VMEM((2, packs, SUBLANES, LANES), f32),
            pltpu.VMEM((packs, SUBLANES, LANES), f32),
            pltpu.VMEM((groups, SUBLANES, LANES), f32),
            pltpu.VMEM((groups, 2, SUBLANES, LANES), f32),
            pltpu.VMEM((groups,) + block, f32),
            pltpu.VMEM((groups,) + block, f32),
            pltpu.VMEM((SUBLANES, LANES), f32),
            pltpu.VMEM((slabs * groups, LANES), f32),
            pltpu.VMEM((groups, shots, owned, cols, slab), f32),
            dma,
            dma,
            regular((groups,)),
            regular,
            dma((2,)),
            dma((2,)),
            dma,
            dma((groups,)),
            dma((min(EARLY, groups),)),
            dma,
            dma,
            dma,
        ],
        compiler_params=pltpu.CompilerParams(collective_id=0, has_side_effects=True),
    )(correlation, illumination, aperture)


def solution(mesh):
    return jax.shard_map(
        on_device,
        mesh=mesh,
        in_specs=(P("shot", None, None, "depth"), P("shot", None, None, "depth"), P("shot", None)),
        out_specs=P("shot", None, "depth"),
        check_vma=False,
    )
```

```python
import functools
import math

import jax
import jax.numpy as jnp
from jax import lax
from jax.experimental import pallas as pl
from jax.experimental.pallas import tpu as pltpu
from jax.sharding import PartitionSpec as P

MESH = pl.DeviceIdType.MESH
LANES = 128
SUBLANES = 8
EARLY = 1


def kernel(dims, corr_hbm, ill_hbm, box_hbm, out_ref, box, raw, norm, centre, edge_out, edge_in, halo_out, halo_in, halves, send, recv, message, inbox, spread,
           ready, passed, edge_send, edge_recv, bulk_send, bulk_recv, halo_recv, note_send, note_recv):
    shots, rows, cols, slab, groups, slabs, owned, cells = dims
    half = cols // 2
    tiles = half // SUBLANES
    devices = groups * slabs
    per_pack = LANES // 2
    per_owner = owned * shots * tiles
    group = lax.axis_index("shot")
    depth = lax.axis_index("depth")
    border = shots * owned * half
    placed = border + 2 * shots * owned
    corr, ill = raw.at[0], raw.at[1]

    box_copy = pltpu.make_async_copy(box_hbm, box, bulk_send)
    box_copy.start()
    for s in range(shots):
        for source, target in ((corr_hbm, corr), (ill_hbm, ill)):
            pltpu.make_async_copy(source.at[s], target.at[s], note_send).start()

    def signal(semaphore, **device):
        pl.semaphore_signal(semaphore, inc=1, device_id=device, device_id_type=MESH)

    def each(low, high, action):
        lax.fori_loop(low, high, lambda t, carry: (action(t), carry)[1], 0)

    barrier = pltpu.get_barrier_semaphore()
    each(1, slabs, lambda d: signal(barrier, depth=lax.rem(depth + d, slabs)))
    each(group + 1, groups, lambda g: signal(barrier, shot=g))

    lane = lax.broadcasted_iota(jnp.int32, (SUBLANES, LANES), 1)
    sub = lax.broadcasted_iota(jnp.int32, (SUBLANES, LANES), 0)
    zero = jnp.zeros((SUBLANES, slab), jnp.float32)
    for s in range(shots):
        for r in (0, rows + 1):
            for t in range(tiles + 2):
                norm[s, r, pl.ds(t * SUBLANES, SUBLANES)] = zero
    packs = edge_out.shape[0]

    @pl.when(depth == 0)
    def _():
        for p in range(packs):
            edge_in[0, p] = zero

    @pl.when(depth == slabs - 1)
    def _():
        for p in range(packs):
            edge_in[1, p] = zero

    box_copy.wait()
    lower = []
    upper = []
    start = []
    for s in range(shots):
        first, last = box[s, 2], box[s, 3]
        start.append(jnp.minimum(first, half))
        lower.append([(sub + t * SUBLANES >= first) & (sub + t * SUBLANES < last) for t in range(tiles)])
        upper.append([(sub + t * SUBLANES + half >= first) & (sub + t * SUBLANES + half < last) for t in range(tiles)])
    pltpu.make_async_copy(raw, raw, note_send).wait()

    def lane_of(r, s, t):
        k = (r * shots + s) * tiles + t
        return k // per_pack, 2 * (k % per_pack)

    packed = [zero] * packs
    for r in range(rows):
        for s in range(shots):
            in_row = (r >= box[s, 0]) & (r < box[s, 1])
            parts = []
            for t in range(tiles):
                here = pl.ds(t * SUBLANES, SUBLANES)
                there = pl.ds(t * SUBLANES + half, SUBLANES)
                top = jnp.where(upper[s][t], corr[s, r, there], corr[s, r, here])
                top = jnp.where((lower[s][t] | upper[s][t]) & in_row, top, 0.0)
                value = top / (jnp.where(upper[s][t], ill[s, r, there], ill[s, r, here]) + 0.1)
                parts.append(value)
                p, k = lane_of(r, s, t)
                packed[p] = jnp.where(lane // 2 == k // 2, pltpu.roll(value, k + 1, 1), packed[p])
            for t, value in enumerate([parts[-1]] + parts + [parts[0]]):
                norm[s, r + 1, pl.ds(t * SUBLANES, SUBLANES)] = value
    for p in range(packs):
        edge_out[p] = packed[p]

    def edge_copy(side):
        return pltpu.make_async_remote_copy(
            src_ref=edge_out, dst_ref=edge_in.at[1 - side], send_sem=edge_send,
            recv_sem=edge_recv, device_id={"depth": depth + (1 if side else -1)}, device_id_type=MESH)

    pl.semaphore_wait(barrier, group + slabs - 1)

    @pl.when(depth > 0)
    def _():
        edge_copy(0).start()

    @pl.when(depth < slabs - 1)
    def _():
        edge_copy(1).start()

    each(0, group, lambda g: signal(ready.at[group - 1], shot=g))
    each(1, slabs, lambda d: signal(passed, depth=lax.rem(depth + d, slabs)))

    row_index = lax.broadcasted_iota(jnp.int32, (rows, slab), 0)
    energies = []
    for s in range(shots):
        in_rows = (row_index >= box[s, 0]) & (row_index < box[s, 1])
        energy = None
        for side, column in enumerate((start[s], start[s] + half - 1)):
            in_box = (column >= box[s, 2]) & (column < box[s, 3])
            value = jnp.where(in_rows & in_box, corr[s, :, column], 0.0) / (ill[s, :, column] + 0.1)
            for owner in range(groups):
                send[owner, pl.ds(border + (2 * s + side) * owned, owned)] = 0.0 - value[owner * owned:(owner + 1) * owned]
            in_grid = (start[s] > 0) if side == 0 else (start[s] < cols - half)
            kept = jnp.where(in_grid, value, 0.0)
            kept = kept * kept
            energy = kept if energy is None else energy + kept
        while energy.shape[0] > SUBLANES:
            energy = energy[:energy.shape[0] // 2] + energy[energy.shape[0] // 2:]
        energies.append(energy)
        for owner in range(groups):
            send[owner, pl.ds(placed + s, 1)] = jnp.full((1, LANES), start[s].astype(jnp.float32))

    for r in range(rows):
        for s in range(shots):
            for t in range(tiles):
                value = norm[s, r + 1, pl.ds((t + 1) * SUBLANES, SUBLANES)]
                beside = jnp.where(lane > 0, pltpu.roll(value, 1, 1), 0.0)
                beside = beside + jnp.where(lane < LANES - 1, pltpu.roll(value, LANES - 1, 1), 0.0)
                centre[s, r, pl.ds(t * SUBLANES, SUBLANES)] = 6.0 * value - beside

    no_before = [[sub + t * SUBLANES == lax.rem(start[s], half) for t in range(tiles)] for s in range(shots)]
    no_after = [[sub + t * SUBLANES == lax.rem(start[s] + half - 1, half) for t in range(tiles)] for s in range(shots)]
    packed = [zero] * packs
    for r in range(rows):
        owner, i = r // owned, r % owned
        for s in range(shots):
            for t in range(tiles):
                base = SUBLANES + t * SUBLANES
                beside = norm[s, r, pl.ds(base, SUBLANES)] + norm[s, r + 2, pl.ds(base, SUBLANES)]
                beside = beside + jnp.where(no_before[s][t], 0.0, norm[s, r + 1, pl.ds(base - 1, SUBLANES)])
                beside = beside + jnp.where(no_after[s][t], 0.0, norm[s, r + 1, pl.ds(base + 1, SUBLANES)])
                p, k = lane_of(r, s, t)
                result = centre[s, r, pl.ds(t * SUBLANES, SUBLANES)] - beside
                energies[s] = energies[s] + result * result
                packed[p] = jnp.where(lane // 2 == k // 2, pltpu.roll(result, k + 1, 1), packed[p])
                send[owner, pl.ds((s * owned + i) * half + t * SUBLANES, SUBLANES)] = result

    def bulk(g, origin):
        return pltpu.make_async_remote_copy(
            src_ref=send.at[g], dst_ref=recv.at[origin], send_sem=bulk_send, recv_sem=bulk_recv.at[lax.div(origin, 2)],
            device_id={"shot": g}, device_id_type=MESH)

    def halo_copy(g):
        return pltpu.make_async_remote_copy(
            src_ref=halo_out.at[g * per_owner // per_pack], dst_ref=halo_in.at[group], send_sem=edge_send,
            recv_sem=halo_recv, device_id={"shot": g}, device_id_type=MESH)

    early = min(EARLY, groups)
    for g in range(early):
        @pl.when(g < group)
        def _():
            bulk(g, group).start()

    for inner, count in ((True, 2), (False, 1)):
        @pl.when(((depth > 0) & (depth < slabs - 1)) == inner)
        def _():
            tile = edge_in.at[pl.ds(0, count)]
            pltpu.make_async_copy(tile, tile, edge_send).wait()
            pltpu.make_async_copy(tile, tile, edge_recv).wait()

    lane_shot = lax.rem(lane // (2 * tiles), shots)
    halos = []
    for p in range(packs):
        halo = jnp.where(lane % 2 == 0, pltpu.roll(edge_in[1, p], LANES - 1, 1), pltpu.roll(edge_in[0, p], 1, 1))
        halo_out[p] = halo
        halos.append(halo)
        change = halo * (halo - 2.0 * packed[p])
        for s in range(shots):
            energies[s] = energies[s] + jnp.where(lane_shot == s, change, 0.0)

    ends = (lane == 0) | (lane == LANES - 1)
    for owner in range(early, groups):
        for i in range(owned):
            for s in range(shots):
                for t in range(tiles):
                    p, k = lane_of(owner * owned + i, s, t)
                    here = pl.ds((s * owned + i) * half + t * SUBLANES, SUBLANES)
                    moved = pltpu.roll(halos[p], LANES - 1 - k, 1)
                    send[owner, here] = send[owner, here] - jnp.where(ends, moved, 0.0)

    def total(value):
        return jnp.sum(jnp.sum(value, axis=0, keepdims=True), axis=1, keepdims=True)

    note = jnp.zeros((1, LANES), jnp.float32)
    gap = LANES // shots
    lane_row = lax.broadcasted_iota(jnp.int32, (1, LANES), 1)
    for s in range(shots):
        note = jnp.where(lane_row // gap == s, total(energies[s]), note)
    message[pl.ds(0, 1)] = note / cells

    slot = depth * groups + group
    own_note = pltpu.make_async_copy(message.at[pl.ds(0, 1)], inbox.at[pl.ds(slot, 1)], note_recv)
    own_note.start()

    def tell(g, d):
        pltpu.make_async_remote_copy(
            src_ref=message.at[pl.ds(0, 1)], dst_ref=inbox.at[pl.ds(slot, 1)], send_sem=note_send, recv_sem=note_recv,
            device_id={"shot": g, "depth": d}, device_id_type=MESH).start()

    pl.semaphore_wait(passed, slabs - 1)
    for g in range(groups):
        @pl.when(g < group)
        def _():
            for d in range(slabs):
                tell(g, d)
    for d in range(slabs):
        @pl.when(d != depth)
        def _():
            tell(group, d)
    for g in range(early):
        @pl.when(g < group)
        def _():
            halo_copy(g).start()
    for g in range(early, groups):
        @pl.when(g < group)
        def _():
            bulk(g, group).start()
    for g in sorted(range(1, groups), key=lambda g: (g % 2, g) if 2 * g >= groups else (2, g)):
        @pl.when(g > group)
        def _():
            pl.semaphore_wait(ready.at[g - 1], 1)
            bulk(g, group).start()
            for d in range(slabs):
                tell(g, d)

    recv[group] = send[group]

    col = [(sub + t * SUBLANES).astype(jnp.float32) for t in range(2 * tiles)]
    for g in range(groups):
        if g % 2 == 0:
            for own, count in ((True, 1), (False, 2)):
                @pl.when((lax.div(group, 2) == g // 2) == own)
                def _():
                    pair = recv.at[pl.ds(g, count)]
                    pltpu.make_async_copy(pair, pair, bulk_recv.at[g // 2]).wait()

        for s in range(shots):
            first = recv[g, pl.ds(placed + s, 1)]
            masks = []
            for t in range(2 * tiles):
                offset = col[t] - first
                masks.append((offset == -1.0, offset == float(half), (offset >= -1.0) & (offset <= float(half))))
            for i in range(owned):
                index = s * owned + i
                low = recv[g, pl.ds(border + 2 * s * owned + i, 1)]
                high = recv[g, pl.ds(border + (2 * s + 1) * owned + i, 1)]
                for t in range(2 * tiles):
                    at_low, at_high, inside = masks[t]
                    value = recv[g, pl.ds(index * half + (t % tiles) * SUBLANES, SUBLANES)]
                    value = jnp.where(at_low, low, jnp.where(at_high, high, value))
                    spread[g, s, i, pl.ds(t * SUBLANES, SUBLANES)] = jnp.where(inside, value, 0.0)

    arrived = halo_in.at[pl.ds(0, groups - 1)]

    @pl.when(group < early)
    def _():
        halo_in[group] = halo_out[lax.div(group * per_owner, per_pack)]
        pltpu.make_async_copy(arrived, arrived, halo_recv).wait()
        fold_col = (lax.rem(lane // 2, tiles) * SUBLANES + sub).astype(jnp.float32)
        for g in range(groups):
            first = recv[g, pl.ds(placed, 1)]
            for s in range(1, shots):
                first = jnp.where(lane_shot == s, recv[g, pl.ds(placed + s, 1)], first)
            halo = halo_in[g]
            halves[g, 0] = jnp.where(fold_col >= first, halo, 0.0)
            halves[g, 1] = jnp.where(fold_col >= first, 0.0, halo)

    pltpu.make_async_copy(inbox, inbox, note_recv).wait()
    meansq = inbox[pl.ds(0, groups)]
    for d in range(1, slabs):
        meansq = meansq + inbox[pl.ds(d * groups, groups)]
    lane_group = lax.broadcasted_iota(jnp.int32, (groups, LANES), 1) // gap
    turned = [meansq] + [pltpu.roll(meansq, j * gap, 1) for j in range(1, shots)]
    by_shot = []
    for s in range(shots):
        value = meansq
        for j in range(1, shots):
            value = jnp.where(lane_group == (s + j) % shots, turned[j], value)
        by_shot.append(value)
    peak = by_shot[0]
    for s in range(1, shots):
        peak = jnp.maximum(peak, by_shot[s])
    peak = 0.5 * jnp.max(peak, axis=0, keepdims=True) + 1.0
    factors = [(1.0 / math.sqrt(shots * groups)) / jnp.sqrt(by_shot[s] + peak) for s in range(shots)]
    for i in range(owned):
        for t in range(2 * tiles):
            total_t = None
            for s in range(shots):
                part = factors[s][0:1] * spread[0, s, i, pl.ds(t * SUBLANES, SUBLANES)]
                for g in range(1, groups):
                    part = part + factors[s][g:g + 1] * spread[g, s, i, pl.ds(t * SUBLANES, SUBLANES)]
                total_t = part if total_t is None else total_t + part
            out_ref[i, pl.ds(t * SUBLANES, SUBLANES)] = total_t

    @pl.when(group < early)
    def _():
        factor = factors[0]
        lane_row_shot = lax.rem(lax.broadcasted_iota(jnp.int32, (groups, LANES), 1) // (2 * tiles), shots)
        for s in range(1, shots):
            factor = jnp.where(lane_row_shot == s, factors[s], factor)
        origin = 2 * lax.rem(group * per_owner, per_pack) + 1
        for h in range(2):
            halo = factor[0:1] * halves[0, h]
            for g in range(1, groups):
                halo = halo + factor[g:g + 1] * halves[g, h]
            for i in range(owned):
                for t in range(tiles):
                    value = None
                    for s in range(shots):
                        shift = 2 * LANES - origin - 2 * ((i * shots + s) * tiles + t)
                        moved = pltpu.roll(halo, shift, 1)
                        value = moved if value is None else value + moved
                    here = pl.ds((h * tiles + t) * SUBLANES, SUBLANES)
                    out_ref[i, here] = out_ref[i, here] - jnp.where(ends, value, 0.0)

    pltpu.make_async_copy(inbox.at[pl.ds(0, devices - 1)], inbox.at[pl.ds(0, devices - 1)], note_send).wait()
    for g in range(early):
        sent = min(g + 1, early)

        @pl.when((group == g + 1) if g + 1 < early else (group > g))
        def _():
            pltpu.make_async_copy(halo_in.at[pl.ds(0, sent)], halo_in.at[pl.ds(0, sent)], edge_send).wait()
    others = send.at[pl.ds(0, groups - 1)]
    pltpu.make_async_copy(others, others, bulk_send).wait()


def on_device(correlation, illumination, aperture):
    shots, rows, cols, slab = correlation.shape
    groups = lax.axis_size("shot")
    slabs = lax.axis_size("depth")
    owned = rows // groups
    half = cols // 2
    tiles = half // SUBLANES
    dims = (shots, rows, cols, slab, groups, slabs, owned, rows * cols * slab * slabs)
    packs = -(-rows * shots * tiles // (LANES // 2))
    block = (shots * owned * (half + 2) + shots, slab)
    f32 = jnp.float32
    dma = pltpu.SemaphoreType.DMA
    regular = pltpu.SemaphoreType.REGULAR
    return pl.pallas_call(
        functools.partial(kernel, dims),
        out_shape=pltpu.VMEM((owned, cols, slab), f32),
        in_specs=[pl.BlockSpec(memory_space=pl.ANY)] * 3,
        out_specs=pl.BlockSpec(memory_space=pltpu.VMEM),
        scratch_shapes=[
            pltpu.SMEM(aperture.shape, jnp.int32),
            pltpu.VMEM((2, shots, rows, cols, slab), f32),
            pltpu.VMEM((shots, rows + 2, half + 2 * SUBLANES, slab), f32),
            pltpu.VMEM((shots, rows, half, slab), f32),
            pltpu.VMEM((packs, SUBLANES, LANES), f32),
            pltpu.VMEM((2, packs, SUBLANES, LANES), f32),
            pltpu.VMEM((packs, SUBLANES, LANES), f32),
            pltpu.VMEM((groups, SUBLANES, LANES), f32),
            pltpu.VMEM((groups, 2, SUBLANES, LANES), f32),
            pltpu.VMEM((groups,) + block, f32),
            pltpu.VMEM((groups,) + block, f32),
            pltpu.VMEM((SUBLANES, LANES), f32),
            pltpu.VMEM((slabs * groups, LANES), f32),
            pltpu.VMEM((groups, shots, owned, cols, slab), f32),
            regular((groups - 1,)),
            regular,
            dma,
            dma,
            dma,
            dma((groups // 2,)),
            dma,
            dma,
            dma,
        ],
        compiler_params=pltpu.CompilerParams(collective_id=0, has_side_effects=True),
    )(correlation, illumination, aperture)


def solution(mesh):
    return jax.shard_map(
        on_device,
        mesh=mesh,
        in_specs=(P("shot", None, None, "depth"), P("shot", None, None, "depth"), P("shot", None)),
        out_specs=P("shot", None, "depth"),
        check_vma=False,
    )
```

```python
import functools
import math

import jax
import jax.numpy as jnp
from jax import lax
from jax.experimental import pallas as pl
from jax.experimental.pallas import tpu as pltpu
from jax.sharding import PartitionSpec as P

MESH = pl.DeviceIdType.MESH
LANES = 128
SUBLANES = 8
EARLY = 1


def kernel(dims, corr_hbm, ill_hbm, box_hbm, out_ref, box, raw, norm, centre, edge_out, edge_in, halo_out, halo_in, halves, spare, send, recv, message, inbox, spread,
           ready, passed, edge_send, edge_recv, bulk_send, bulk_recv, halo_recv, note_send, note_recv):
    shots, rows, cols, slab, groups, slabs, owned, cells = dims
    half = cols // 2
    tiles = half // SUBLANES
    devices = groups * slabs
    per_pack = LANES // 2
    per_owner = owned * shots * tiles
    group = lax.axis_index("shot")
    depth = lax.axis_index("depth")
    border = shots * owned * half
    placed = border + 2 * shots * owned
    corr, ill = raw.at[0], raw.at[1]

    box_copy = pltpu.make_async_copy(box_hbm, box, bulk_send)
    box_copy.start()
    for s in range(shots):
        for source, target in ((corr_hbm, corr), (ill_hbm, ill)):
            pltpu.make_async_copy(source.at[s], target.at[s], note_send).start()

    def signal(semaphore, **device):
        pl.semaphore_signal(semaphore, inc=1, device_id=device, device_id_type=MESH)

    def each(low, high, action):
        lax.fori_loop(low, high, lambda t, carry: (action(t), carry)[1], 0)

    barrier = pltpu.get_barrier_semaphore()
    each(1, slabs, lambda d: signal(barrier, depth=lax.rem(depth + d, slabs)))
    each(group + 1, groups, lambda g: signal(barrier, shot=g))

    lane = lax.broadcasted_iota(jnp.int32, (SUBLANES, LANES), 1)
    sub = lax.broadcasted_iota(jnp.int32, (SUBLANES, LANES), 0)
    zero = jnp.zeros((SUBLANES, slab), jnp.float32)
    for s in range(shots):
        for r in (0, rows + 1):
            for t in range(tiles + 2):
                norm[s, r, pl.ds(t * SUBLANES, SUBLANES)] = zero
    packs = edge_out.shape[0]

    @pl.when(depth == 0)
    def _():
        for p in range(packs):
            edge_in[0, p] = zero

    @pl.when(depth == slabs - 1)
    def _():
        for p in range(packs):
            edge_in[1, p] = zero

    box_copy.wait()
    lower = []
    upper = []
    start = []
    for s in range(shots):
        first, last = box[s, 2], box[s, 3]
        start.append(jnp.minimum(first, half))
        lower.append([(sub + t * SUBLANES >= first) & (sub + t * SUBLANES < last) for t in range(tiles)])
        upper.append([(sub + t * SUBLANES + half >= first) & (sub + t * SUBLANES + half < last) for t in range(tiles)])
    pltpu.make_async_copy(raw, raw, note_send).wait()

    def lane_of(r, s, t):
        k = (r * shots + s) * tiles + t
        return k // per_pack, 2 * (k % per_pack)

    packed = [zero] * packs
    for r in range(rows):
        for s in range(shots):
            in_row = (r >= box[s, 0]) & (r < box[s, 1])
            parts = []
            for t in range(tiles):
                here = pl.ds(t * SUBLANES, SUBLANES)
                there = pl.ds(t * SUBLANES + half, SUBLANES)
                top = jnp.where(upper[s][t], corr[s, r, there], corr[s, r, here])
                top = jnp.where((lower[s][t] | upper[s][t]) & in_row, top, 0.0)
                value = top / (jnp.where(upper[s][t], ill[s, r, there], ill[s, r, here]) + 0.1)
                parts.append(value)
                p, k = lane_of(r, s, t)
                packed[p] = jnp.where(lane // 2 == k // 2, pltpu.roll(value, k + 1, 1), packed[p])
            for t, value in enumerate([parts[-1]] + parts + [parts[0]]):
                norm[s, r + 1, pl.ds(t * SUBLANES, SUBLANES)] = value
    for p in range(packs):
        edge_out[p] = packed[p]

    def edge_copy(side):
        return pltpu.make_async_remote_copy(
            src_ref=edge_out, dst_ref=edge_in.at[1 - side], send_sem=edge_send,
            recv_sem=edge_recv, device_id={"depth": depth + (1 if side else -1)}, device_id_type=MESH)

    def laplacian():
        row_index = lax.broadcasted_iota(jnp.int32, (rows, slab), 0)
        energies = []
        for s in range(shots):
            in_rows = (row_index >= box[s, 0]) & (row_index < box[s, 1])
            energy = None
            for side, column in enumerate((start[s], start[s] + half - 1)):
                in_box = (column >= box[s, 2]) & (column < box[s, 3])
                value = jnp.where(in_rows & in_box, corr[s, :, column], 0.0) / (ill[s, :, column] + 0.1)
                for owner in range(groups):
                    send[owner, pl.ds(border + (2 * s + side) * owned, owned)] = 0.0 - value[owner * owned:(owner + 1) * owned]
                in_grid = (start[s] > 0) if side == 0 else (start[s] < cols - half)
                kept = jnp.where(in_grid, value, 0.0)
                kept = kept * kept
                energy = kept if energy is None else energy + kept
            while energy.shape[0] > SUBLANES:
                energy = energy[:energy.shape[0] // 2] + energy[energy.shape[0] // 2:]
            energies.append(energy)
            for owner in range(groups):
                send[owner, pl.ds(placed + s, 1)] = jnp.full((1, LANES), start[s].astype(jnp.float32))

        for r in range(rows):
            for s in range(shots):
                for t in range(tiles):
                    value = norm[s, r + 1, pl.ds((t + 1) * SUBLANES, SUBLANES)]
                    beside = jnp.where(lane > 0, pltpu.roll(value, 1, 1), 0.0)
                    beside = beside + jnp.where(lane < LANES - 1, pltpu.roll(value, LANES - 1, 1), 0.0)
                    centre[s, r, pl.ds(t * SUBLANES, SUBLANES)] = 6.0 * value - beside

        no_before = [[sub + t * SUBLANES == lax.rem(start[s], half) for t in range(tiles)] for s in range(shots)]
        no_after = [[sub + t * SUBLANES == lax.rem(start[s] + half - 1, half) for t in range(tiles)] for s in range(shots)]
        packed = [zero] * packs
        for r in range(rows):
            owner, i = r // owned, r % owned
            for s in range(shots):
                for t in range(tiles):
                    base = SUBLANES + t * SUBLANES
                    beside = norm[s, r, pl.ds(base, SUBLANES)] + norm[s, r + 2, pl.ds(base, SUBLANES)]
                    beside = beside + jnp.where(no_before[s][t], 0.0, norm[s, r + 1, pl.ds(base - 1, SUBLANES)])
                    beside = beside + jnp.where(no_after[s][t], 0.0, norm[s, r + 1, pl.ds(base + 1, SUBLANES)])
                    p, k = lane_of(r, s, t)
                    result = centre[s, r, pl.ds(t * SUBLANES, SUBLANES)] - beside
                    energies[s] = energies[s] + result * result
                    packed[p] = jnp.where(lane // 2 == k // 2, pltpu.roll(result, k + 1, 1), packed[p])
                    send[owner, pl.ds((s * owned + i) * half + t * SUBLANES, SUBLANES)] = result
        return tuple(energies) + tuple(packed)

    late = (lax.rem(depth, 2) == 1) & (depth < slabs - 1)
    before = lax.cond(late, laplacian, lambda: (zero,) * (shots + packs))

    pl.semaphore_wait(barrier, group + slabs - 1)

    @pl.when(depth > 0)
    def _():
        edge_copy(0).start()

    @pl.when(depth < slabs - 1)
    def _():
        edge_copy(1).start()

    each(0, group, lambda g: signal(ready.at[group - 1], shot=g))
    each(1, slabs, lambda d: signal(passed, depth=lax.rem(depth + d, slabs)))

    after = lax.cond(late, lambda: before, laplacian)
    energies, packed = list(after[:shots]), list(after[shots:])

    def bulk(g, origin):
        return pltpu.make_async_remote_copy(
            src_ref=send.at[g], dst_ref=recv.at[origin], send_sem=bulk_send, recv_sem=bulk_recv.at[lax.div(origin, 2)],
            device_id={"shot": g}, device_id_type=MESH)

    def halo_copy(g):
        return pltpu.make_async_remote_copy(
            src_ref=halo_out.at[g * per_owner // per_pack], dst_ref=halo_in.at[group], send_sem=edge_send,
            recv_sem=halo_recv, device_id={"shot": g}, device_id_type=MESH)

    early = min(EARLY, groups)
    for g in range(early):
        @pl.when(g < group)
        def _():
            bulk(g, group).start()

    quarter = groups // 4
    pairs = ((range(quarter, 2 * quarter), 2 * quarter), (range(2 * quarter, 3 * quarter), quarter))
    ahead = [late & (group >= sources[0]) & (group <= sources[-1]) for sources, target in pairs]
    any_ahead = ahead[0] | ahead[1]
    for here, (sources, target) in zip(ahead, pairs):
        @pl.when(here)
        def _():
            spare[...] = send[target]
            if target > sources[0]:
                pl.semaphore_wait(ready.at[target - 1], 1)
            pltpu.make_async_remote_copy(
                src_ref=spare, dst_ref=recv.at[group], send_sem=bulk_send, recv_sem=bulk_recv.at[lax.div(group, 2)],
                device_id={"shot": target}, device_id_type=MESH).start()

    for inner, count in ((True, 2), (False, 1)):
        @pl.when(((depth > 0) & (depth < slabs - 1)) == inner)
        def _():
            tile = edge_in.at[pl.ds(0, count)]
            pltpu.make_async_copy(tile, tile, edge_send).wait()
            pltpu.make_async_copy(tile, tile, edge_recv).wait()

    lane_shot = lax.rem(lane // (2 * tiles), shots)
    halos = []
    for p in range(packs):
        halo = jnp.where(lane % 2 == 0, pltpu.roll(edge_in[1, p], LANES - 1, 1), pltpu.roll(edge_in[0, p], 1, 1))
        halo_out[p] = halo
        halos.append(halo)
        change = halo * (halo - 2.0 * packed[p])
        for s in range(shots):
            energies[s] = energies[s] + jnp.where(lane_shot == s, change, 0.0)

    ends = (lane == 0) | (lane == LANES - 1)
    for owner in range(early, groups):
        for i in range(owned):
            for s in range(shots):
                for t in range(tiles):
                    p, k = lane_of(owner * owned + i, s, t)
                    here = pl.ds((s * owned + i) * half + t * SUBLANES, SUBLANES)
                    moved = pltpu.roll(halos[p], LANES - 1 - k, 1)
                    send[owner, here] = send[owner, here] - jnp.where(ends, moved, 0.0)

    def total(value):
        return jnp.sum(jnp.sum(value, axis=0, keepdims=True), axis=1, keepdims=True)

    note = jnp.zeros((1, LANES), jnp.float32)
    gap = LANES // shots
    lane_row = lax.broadcasted_iota(jnp.int32, (1, LANES), 1)
    for s in range(shots):
        note = jnp.where(lane_row // gap == s, total(energies[s]), note)
    message[pl.ds(0, 1)] = note / cells

    slot = depth * groups + group
    own_note = pltpu.make_async_copy(message.at[pl.ds(0, 1)], inbox.at[pl.ds(slot, 1)], note_recv)
    own_note.start()

    def tell(g, d):
        pltpu.make_async_remote_copy(
            src_ref=message.at[pl.ds(0, 1)], dst_ref=inbox.at[pl.ds(slot, 1)], send_sem=note_send, recv_sem=note_recv,
            device_id={"shot": g, "depth": d}, device_id_type=MESH).start()

    pl.semaphore_wait(passed, slabs - 1)
    for g in range(groups):
        @pl.when(g < group)
        def _():
            for d in range(slabs):
                tell(g, d)
    for d in range(slabs):
        @pl.when(d != depth)
        def _():
            tell(group, d)
    for g in range(early):
        @pl.when(g < group)
        def _():
            halo_copy(g).start()

    for here, (sources, target) in zip(ahead, pairs):
        @pl.when(here)
        def _():
            halo_copy(target).start()

    for g in range(early, groups):
        @pl.when((g < group) & jnp.logical_not(ahead[1] & (g == pairs[1][1])))
        def _():
            bulk(g, group).start()
    for g in sorted(range(1, groups), key=lambda g: (g % 2, g) if 2 * g >= groups else (2, g)):
        @pl.when(g > group)
        def _():
            if g == pairs[0][1]:
                @pl.when(jnp.logical_not(ahead[0]))
                def _():
                    pl.semaphore_wait(ready.at[g - 1], 1)
                    bulk(g, group).start()
            else:
                pl.semaphore_wait(ready.at[g - 1], 1)
                bulk(g, group).start()
            for d in range(slabs):
                tell(g, d)

    recv[group] = send[group]

    col = [(sub + t * SUBLANES).astype(jnp.float32) for t in range(2 * tiles)]
    for g in range(groups):
        if g % 2 == 0:
            for own, count in ((True, 1), (False, 2)):
                @pl.when((lax.div(group, 2) == g // 2) == own)
                def _():
                    pair = recv.at[pl.ds(g, count)]
                    pltpu.make_async_copy(pair, pair, bulk_recv.at[g // 2]).wait()

        for s in range(shots):
            first = recv[g, pl.ds(placed + s, 1)]
            masks = []
            for t in range(2 * tiles):
                offset = col[t] - first
                masks.append((offset == -1.0, offset == float(half), (offset >= -1.0) & (offset <= float(half))))
            for i in range(owned):
                index = s * owned + i
                low = recv[g, pl.ds(border + 2 * s * owned + i, 1)]
                high = recv[g, pl.ds(border + (2 * s + 1) * owned + i, 1)]
                for t in range(2 * tiles):
                    at_low, at_high, inside = masks[t]
                    value = recv[g, pl.ds(index * half + (t % tiles) * SUBLANES, SUBLANES)]
                    value = jnp.where(at_low, low, jnp.where(at_high, high, value))
                    spread[g, s, i, pl.ds(t * SUBLANES, SUBLANES)] = jnp.where(inside, value, 0.0)

    def collect(sources, count):
        arrived = halo_in.at[pl.ds(0, count)]
        pltpu.make_async_copy(arrived, arrived, halo_recv).wait()
        fold_col = (lax.rem(lane // 2, tiles) * SUBLANES + sub).astype(jnp.float32)
        for g in sources:
            first = recv[g, pl.ds(placed, 1)]
            for s in range(1, shots):
                first = jnp.where(lane_shot == s, recv[g, pl.ds(placed + s, 1)], first)
            halo = halo_in[g]
            halves[g, 0] = jnp.where(fold_col >= first, halo, 0.0)
            halves[g, 1] = jnp.where(fold_col >= first, 0.0, halo)

    @pl.when(group < early)
    def _():
        halo_in[group] = halo_out[lax.div(group * per_owner, per_pack)]
        collect(range(groups), groups - 1)

    for sources, target in pairs:
        @pl.when(late & (group == target))
        def _():
            collect(sources, len(sources))

    pltpu.make_async_copy(inbox, inbox, note_recv).wait()
    meansq = inbox[pl.ds(0, groups)]
    for d in range(1, slabs):
        meansq = meansq + inbox[pl.ds(d * groups, groups)]
    lane_group = lax.broadcasted_iota(jnp.int32, (groups, LANES), 1) // gap
    turned = [meansq] + [pltpu.roll(meansq, j * gap, 1) for j in range(1, shots)]
    by_shot = []
    for s in range(shots):
        value = meansq
        for j in range(1, shots):
            value = jnp.where(lane_group == (s + j) % shots, turned[j], value)
        by_shot.append(value)
    peak = by_shot[0]
    for s in range(1, shots):
        peak = jnp.maximum(peak, by_shot[s])
    peak = 0.5 * jnp.max(peak, axis=0, keepdims=True) + 1.0
    factors = [(1.0 / math.sqrt(shots * groups)) / jnp.sqrt(by_shot[s] + peak) for s in range(shots)]
    for i in range(owned):
        for t in range(2 * tiles):
            total_t = None
            for s in range(shots):
                part = factors[s][0:1] * spread[0, s, i, pl.ds(t * SUBLANES, SUBLANES)]
                for g in range(1, groups):
                    part = part + factors[s][g:g + 1] * spread[g, s, i, pl.ds(t * SUBLANES, SUBLANES)]
                total_t = part if total_t is None else total_t + part
            out_ref[i, pl.ds(t * SUBLANES, SUBLANES)] = total_t

    def correct(sources):
        factor = factors[0]
        lane_row_shot = lax.rem(lax.broadcasted_iota(jnp.int32, (groups, LANES), 1) // (2 * tiles), shots)
        for s in range(1, shots):
            factor = jnp.where(lane_row_shot == s, factors[s], factor)
        origin = 2 * lax.rem(group * per_owner, per_pack) + 1
        for h in range(2):
            halo = zero
            for g in sources:
                halo = halo + factor[g:g + 1] * halves[g, h]
            for i in range(owned):
                for t in range(tiles):
                    value = None
                    for s in range(shots):
                        shift = 2 * LANES - origin - 2 * ((i * shots + s) * tiles + t)
                        moved = pltpu.roll(halo, shift, 1)
                        value = moved if value is None else value + moved
                    here = pl.ds((h * tiles + t) * SUBLANES, SUBLANES)
                    out_ref[i, here] = out_ref[i, here] - jnp.where(ends, value, 0.0)

    @pl.when(group < early)
    def _():
        correct(range(groups))

    for sources, target in pairs:
        @pl.when(late & (group == target))
        def _():
            correct(sources)

    pltpu.make_async_copy(inbox.at[pl.ds(0, devices - 1)], inbox.at[pl.ds(0, devices - 1)], note_send).wait()
    for g in range(early):
        for extra in (False, True):
            sent = min(g + 1, early) + extra

            @pl.when(((group == g + 1) if g + 1 < early else (group > g)) & (any_ahead == extra))
            def _():
                pltpu.make_async_copy(halo_in.at[pl.ds(0, sent)], halo_in.at[pl.ds(0, sent)], edge_send).wait()

    others = send.at[pl.ds(0, groups - 1)]
    pltpu.make_async_copy(others, others, bulk_send).wait()


def on_device(correlation, illumination, aperture):
    shots, rows, cols, slab = correlation.shape
    groups = lax.axis_size("shot")
    slabs = lax.axis_size("depth")
    owned = rows // groups
    half = cols // 2
    tiles = half // SUBLANES
    dims = (shots, rows, cols, slab, groups, slabs, owned, rows * cols * slab * slabs)
    packs = -(-rows * shots * tiles // (LANES // 2))
    block = (shots * owned * (half + 2) + shots, slab)
    f32 = jnp.float32
    dma = pltpu.SemaphoreType.DMA
    regular = pltpu.SemaphoreType.REGULAR
    return pl.pallas_call(
        functools.partial(kernel, dims),
        out_shape=pltpu.VMEM((owned, cols, slab), f32),
        in_specs=[pl.BlockSpec(memory_space=pl.ANY)] * 3,
        out_specs=pl.BlockSpec(memory_space=pltpu.VMEM),
        scratch_shapes=[
            pltpu.SMEM(aperture.shape, jnp.int32),
            pltpu.VMEM((2, shots, rows, cols, slab), f32),
            pltpu.VMEM((shots, rows + 2, half + 2 * SUBLANES, slab), f32),
            pltpu.VMEM((shots, rows, half, slab), f32),
            pltpu.VMEM((packs, SUBLANES, LANES), f32),
            pltpu.VMEM((2, packs, SUBLANES, LANES), f32),
            pltpu.VMEM((packs, SUBLANES, LANES), f32),
            pltpu.VMEM((groups, SUBLANES, LANES), f32),
            pltpu.VMEM((groups, 2, SUBLANES, LANES), f32),
            pltpu.VMEM(block, f32),
            pltpu.VMEM((groups,) + block, f32),
            pltpu.VMEM((groups,) + block, f32),
            pltpu.VMEM((SUBLANES, LANES), f32),
            pltpu.VMEM((slabs * groups, LANES), f32),
            pltpu.VMEM((groups, shots, owned, cols, slab), f32),
            regular((groups - 1,)),
            regular,
            dma,
            dma,
            dma,
            dma((groups // 2,)),
            dma,
            dma,
            dma,
        ],
        compiler_params=pltpu.CompilerParams(collective_id=0, has_side_effects=True),
    )(correlation, illumination, aperture)


def solution(mesh):
    return jax.shard_map(
        on_device,
        mesh=mesh,
        in_specs=(P("shot", None, None, "depth"), P("shot", None, None, "depth"), P("shot", None)),
        out_specs=P("shot", None, "depth"),
        check_vma=False,
    )
```

```python
import functools
import math

import jax
import jax.numpy as jnp
from jax import lax
from jax.experimental import pallas as pl
from jax.experimental.pallas import tpu as pltpu
from jax.sharding import PartitionSpec as P

MESH = pl.DeviceIdType.MESH
LANES = 128
SUBLANES = 8
EARLY = 1


def kernel(dims, corr_hbm, ill_hbm, box_hbm, out_ref, box, raw, norm, centre, edge_out, edge_in, halo_out, halo_in, halves, spare, send, recv, message, inbox, spread,
           ready, passed, edge_send, edge_recv, bulk_send, bulk_recv, halo_recv, note_send, note_recv):
    shots, rows, cols, slab, groups, slabs, owned, cells = dims
    half = cols // 2
    tiles = half // SUBLANES
    devices = groups * slabs
    per_pack = LANES // 2
    per_owner = owned * shots * tiles
    group = lax.axis_index("shot")
    depth = lax.axis_index("depth")
    border = shots * owned * half
    placed = border + 2 * shots * owned
    corr, ill = raw.at[0], raw.at[1]

    box_copy = pltpu.make_async_copy(box_hbm, box, bulk_send)
    box_copy.start()
    for s in range(shots):
        for source, target in ((corr_hbm, corr), (ill_hbm, ill)):
            pltpu.make_async_copy(source.at[s], target.at[s], note_send).start()

    def signal(semaphore, **device):
        pl.semaphore_signal(semaphore, inc=1, device_id=device, device_id_type=MESH)

    def each(low, high, action):
        lax.fori_loop(low, high, lambda t, carry: (action(t), carry)[1], 0)

    barrier = pltpu.get_barrier_semaphore()
    each(1, slabs, lambda d: signal(barrier, depth=lax.rem(depth + d, slabs)))
    each(group + 1, groups, lambda g: signal(barrier, shot=g))

    lane = lax.broadcasted_iota(jnp.int32, (SUBLANES, LANES), 1)
    sub = lax.broadcasted_iota(jnp.int32, (SUBLANES, LANES), 0)
    zero = jnp.zeros((SUBLANES, slab), jnp.float32)
    for s in range(shots):
        for r in (0, rows + 1):
            for t in range(tiles + 2):
                norm[s, r, pl.ds(t * SUBLANES, SUBLANES)] = zero
    packs = edge_out.shape[0]

    @pl.when(depth == 0)
    def _():
        for p in range(packs):
            edge_in[0, p] = zero

    @pl.when(depth == slabs - 1)
    def _():
        for p in range(packs):
            edge_in[1, p] = zero

    box_copy.wait()
    lower = []
    upper = []
    start = []
    for s in range(shots):
        first, last = box[s, 2], box[s, 3]
        start.append(jnp.minimum(first, half))
        lower.append([(sub + t * SUBLANES >= first) & (sub + t * SUBLANES < last) for t in range(tiles)])
        upper.append([(sub + t * SUBLANES + half >= first) & (sub + t * SUBLANES + half < last) for t in range(tiles)])
    pltpu.make_async_copy(raw, raw, note_send).wait()

    def lane_of(r, s, t):
        k = (r * shots + s) * tiles + t
        return k // per_pack, 2 * (k % per_pack)

    packed = [zero] * packs
    for r in range(rows):
        for s in range(shots):
            in_row = (r >= box[s, 0]) & (r < box[s, 1])
            parts = []
            for t in range(tiles):
                here = pl.ds(t * SUBLANES, SUBLANES)
                there = pl.ds(t * SUBLANES + half, SUBLANES)
                top = jnp.where(upper[s][t], corr[s, r, there], corr[s, r, here])
                top = jnp.where((lower[s][t] | upper[s][t]) & in_row, top, 0.0)
                value = top / (jnp.where(upper[s][t], ill[s, r, there], ill[s, r, here]) + 0.1)
                parts.append(value)
                p, k = lane_of(r, s, t)
                packed[p] = jnp.where(lane // 2 == k // 2, pltpu.roll(value, k + 1, 1), packed[p])
            for t, value in enumerate([parts[-1]] + parts + [parts[0]]):
                norm[s, r + 1, pl.ds(t * SUBLANES, SUBLANES)] = value
    for p in range(packs):
        edge_out[p] = packed[p]

    def edge_copy(side):
        return pltpu.make_async_remote_copy(
            src_ref=edge_out, dst_ref=edge_in.at[1 - side], send_sem=edge_send,
            recv_sem=edge_recv, device_id={"depth": depth + (1 if side else -1)}, device_id_type=MESH)

    def laplacian():
        row_index = lax.broadcasted_iota(jnp.int32, (rows, slab), 0)
        energies = []
        for s in range(shots):
            in_rows = (row_index >= box[s, 0]) & (row_index < box[s, 1])
            energy = None
            for side, column in enumerate((start[s], start[s] + half - 1)):
                in_box = (column >= box[s, 2]) & (column < box[s, 3])
                value = jnp.where(in_rows & in_box, corr[s, :, column], 0.0) / (ill[s, :, column] + 0.1)
                for owner in range(groups):
                    send[owner, pl.ds(border + (2 * s + side) * owned, owned)] = 0.0 - value[owner * owned:(owner + 1) * owned]
                in_grid = (start[s] > 0) if side == 0 else (start[s] < cols - half)
                kept = jnp.where(in_grid, value, 0.0)
                kept = kept * kept
                energy = kept if energy is None else energy + kept
            while energy.shape[0] > SUBLANES:
                energy = energy[:energy.shape[0] // 2] + energy[energy.shape[0] // 2:]
            energies.append(energy)
            for owner in range(groups):
                send[owner, pl.ds(placed + s, 1)] = jnp.full((1, LANES), start[s].astype(jnp.float32))

        for r in range(rows):
            for s in range(shots):
                for t in range(tiles):
                    value = norm[s, r + 1, pl.ds((t + 1) * SUBLANES, SUBLANES)]
                    beside = jnp.where(lane > 0, pltpu.roll(value, 1, 1), 0.0)
                    beside = beside + jnp.where(lane < LANES - 1, pltpu.roll(value, LANES - 1, 1), 0.0)
                    centre[s, r, pl.ds(t * SUBLANES, SUBLANES)] = 6.0 * value - beside

        no_before = [[sub + t * SUBLANES == lax.rem(start[s], half) for t in range(tiles)] for s in range(shots)]
        no_after = [[sub + t * SUBLANES == lax.rem(start[s] + half - 1, half) for t in range(tiles)] for s in range(shots)]
        packed = [zero] * packs
        for r in range(rows):
            owner, i = r // owned, r % owned
            for s in range(shots):
                for t in range(tiles):
                    base = SUBLANES + t * SUBLANES
                    beside = norm[s, r, pl.ds(base, SUBLANES)] + norm[s, r + 2, pl.ds(base, SUBLANES)]
                    beside = beside + jnp.where(no_before[s][t], 0.0, norm[s, r + 1, pl.ds(base - 1, SUBLANES)])
                    beside = beside + jnp.where(no_after[s][t], 0.0, norm[s, r + 1, pl.ds(base + 1, SUBLANES)])
                    p, k = lane_of(r, s, t)
                    result = centre[s, r, pl.ds(t * SUBLANES, SUBLANES)] - beside
                    energies[s] = energies[s] + result * result
                    packed[p] = jnp.where(lane // 2 == k // 2, pltpu.roll(result, k + 1, 1), packed[p])
                    send[owner, pl.ds((s * owned + i) * half + t * SUBLANES, SUBLANES)] = result
        return tuple(energies) + tuple(packed)

    late = (lax.rem(depth, 2) == 1) & (depth < slabs - 1)
    before = lax.cond(late, laplacian, lambda: (zero,) * (shots + packs))

    pl.semaphore_wait(barrier, group + slabs - 1)

    @pl.when(depth > 0)
    def _():
        edge_copy(0).start()

    @pl.when(depth < slabs - 1)
    def _():
        edge_copy(1).start()

    each(0, group, lambda g: signal(ready.at[group - 1], shot=g))
    each(1, slabs, lambda d: signal(passed, depth=lax.rem(depth + d, slabs)))

    after = lax.cond(late, lambda: before, laplacian)
    energies, packed = list(after[:shots]), list(after[shots:])

    def bulk(g, origin):
        return pltpu.make_async_remote_copy(
            src_ref=send.at[g], dst_ref=recv.at[origin], send_sem=bulk_send, recv_sem=bulk_recv.at[lax.div(origin, 2)],
            device_id={"shot": g}, device_id_type=MESH)

    def halo_copy(g):
        return pltpu.make_async_remote_copy(
            src_ref=halo_out.at[g * per_owner // per_pack], dst_ref=halo_in.at[group], send_sem=edge_send,
            recv_sem=halo_recv, device_id={"shot": g}, device_id_type=MESH)

    early = min(EARLY, groups)
    for g in range(early):
        @pl.when(g < group)
        def _():
            bulk(g, group).start()

    quarter = groups // 4
    pairs = ((range(quarter, 2 * quarter), 2 * quarter), (range(2 * quarter, 3 * quarter), quarter))
    ahead = [late & (group >= sources[0]) & (group <= sources[-1]) for sources, target in pairs]
    any_ahead = ahead[0] | ahead[1]
    for here, (sources, target) in zip(ahead, pairs):
        @pl.when(here)
        def _():
            spare[...] = send[target]
            if target > sources[0]:
                pl.semaphore_wait(ready.at[target - 1], 1)
            pltpu.make_async_remote_copy(
                src_ref=spare, dst_ref=recv.at[group], send_sem=bulk_send, recv_sem=bulk_recv.at[lax.div(group, 2)],
                device_id={"shot": target}, device_id_type=MESH).start()

    for inner, count in ((True, 2), (False, 1)):
        @pl.when(((depth > 0) & (depth < slabs - 1)) == inner)
        def _():
            tile = edge_in.at[pl.ds(0, count)]
            pltpu.make_async_copy(tile, tile, edge_send).wait()
            pltpu.make_async_copy(tile, tile, edge_recv).wait()

    lane_shot = lax.rem(lane // (2 * tiles), shots)
    halos = []
    for p in range(packs):
        halo = jnp.where(lane % 2 == 0, pltpu.roll(edge_in[1, p], LANES - 1, 1), pltpu.roll(edge_in[0, p], 1, 1))
        halo_out[p] = halo
        halos.append(halo)
        change = halo * (halo - 2.0 * packed[p])
        for s in range(shots):
            energies[s] = energies[s] + jnp.where(lane_shot == s, change, 0.0)

    ends = (lane == 0) | (lane == LANES - 1)
    for owner in range(early, groups):
        for i in range(owned):
            for s in range(shots):
                for t in range(tiles):
                    p, k = lane_of(owner * owned + i, s, t)
                    here = pl.ds((s * owned + i) * half + t * SUBLANES, SUBLANES)
                    moved = pltpu.roll(halos[p], LANES - 1 - k, 1)
                    send[owner, here] = send[owner, here] - jnp.where(ends, moved, 0.0)

    def total(value):
        return jnp.sum(jnp.sum(value, axis=0, keepdims=True), axis=1, keepdims=True)

    note = jnp.zeros((1, LANES), jnp.float32)
    gap = LANES // shots
    lane_row = lax.broadcasted_iota(jnp.int32, (1, LANES), 1)
    for s in range(shots):
        note = jnp.where(lane_row // gap == s, total(energies[s]), note)
    message[pl.ds(0, 1)] = note / cells

    slot = depth * groups + group
    own_note = pltpu.make_async_copy(message.at[pl.ds(0, 1)], inbox.at[pl.ds(slot, 1)], note_recv)
    own_note.start()

    def tell(g, d):
        pltpu.make_async_remote_copy(
            src_ref=message.at[pl.ds(0, 1)], dst_ref=inbox.at[pl.ds(slot, 1)], send_sem=note_send, recv_sem=note_recv,
            device_id={"shot": g, "depth": d}, device_id_type=MESH).start()

    @pl.when((group > early) & (depth == 0))
    def _():
        bulk(early, group).start()

    pl.semaphore_wait(passed, slabs - 1)
    for g in range(groups):
        @pl.when(g < group)
        def _():
            for d in range(slabs):
                tell(g, d)
    for d in range(slabs):
        @pl.when(d != depth)
        def _():
            tell(group, d)
    for g in range(early):
        @pl.when(g < group)
        def _():
            halo_copy(g).start()

    for here, (sources, target) in zip(ahead, pairs):
        @pl.when(here)
        def _():
            halo_copy(target).start()

    for g in range(early, groups):
        @pl.when((g < group) & jnp.logical_not((ahead[1] & (g == pairs[1][1])) | ((depth == 0) & (g == early))))
        def _():
            bulk(g, group).start()
    for g in sorted(range(1, groups), key=lambda g: (g % 2, g) if 2 * g >= groups else (2, g)):
        @pl.when(g > group)
        def _():
            if g == pairs[0][1]:
                @pl.when(jnp.logical_not(ahead[0]))
                def _():
                    pl.semaphore_wait(ready.at[g - 1], 1)
                    bulk(g, group).start()
            else:
                pl.semaphore_wait(ready.at[g - 1], 1)
                bulk(g, group).start()
            for d in range(slabs):
                tell(g, d)

    recv[group] = send[group]

    col = [(sub + t * SUBLANES).astype(jnp.float32) for t in range(2 * tiles)]
    for g in range(groups):
        if g % 2 == 0:
            for own, count in ((True, 1), (False, 2)):
                @pl.when((lax.div(group, 2) == g // 2) == own)
                def _():
                    pair = recv.at[pl.ds(g, count)]
                    pltpu.make_async_copy(pair, pair, bulk_recv.at[g // 2]).wait()

        for s in range(shots):
            first = recv[g, pl.ds(placed + s, 1)]
            masks = []
            for t in range(2 * tiles):
                offset = col[t] - first
                masks.append((offset == -1.0, offset == float(half), (offset >= -1.0) & (offset <= float(half))))
            for i in range(owned):
                index = s * owned + i
                low = recv[g, pl.ds(border + 2 * s * owned + i, 1)]
                high = recv[g, pl.ds(border + (2 * s + 1) * owned + i, 1)]
                for t in range(2 * tiles):
                    at_low, at_high, inside = masks[t]
                    value = recv[g, pl.ds(index * half + (t % tiles) * SUBLANES, SUBLANES)]
                    value = jnp.where(at_low, low, jnp.where(at_high, high, value))
                    spread[g, s, i, pl.ds(t * SUBLANES, SUBLANES)] = jnp.where(inside, value, 0.0)

    def collect(sources, count):
        arrived = halo_in.at[pl.ds(0, count)]
        pltpu.make_async_copy(arrived, arrived, halo_recv).wait()
        fold_col = (lax.rem(lane // 2, tiles) * SUBLANES + sub).astype(jnp.float32)
        for g in sources:
            first = recv[g, pl.ds(placed, 1)]
            for s in range(1, shots):
                first = jnp.where(lane_shot == s, recv[g, pl.ds(placed + s, 1)], first)
            halo = halo_in[g]
            halves[g, 0] = jnp.where(fold_col >= first, halo, 0.0)
            halves[g, 1] = jnp.where(fold_col >= first, 0.0, halo)

    @pl.when(group < early)
    def _():
        halo_in[group] = halo_out[lax.div(group * per_owner, per_pack)]
        collect(range(groups), groups - 1)

    for sources, target in pairs:
        @pl.when(late & (group == target))
        def _():
            collect(sources, len(sources))

    pltpu.make_async_copy(inbox, inbox, note_recv).wait()
    meansq = inbox[pl.ds(0, groups)]
    for d in range(1, slabs):
        meansq = meansq + inbox[pl.ds(d * groups, groups)]
    lane_group = lax.broadcasted_iota(jnp.int32, (groups, LANES), 1) // gap
    turned = [meansq] + [pltpu.roll(meansq, j * gap, 1) for j in range(1, shots)]
    by_shot = []
    for s in range(shots):
        value = meansq
        for j in range(1, shots):
            value = jnp.where(lane_group == (s + j) % shots, turned[j], value)
        by_shot.append(value)
    peak = by_shot[0]
    for s in range(1, shots):
        peak = jnp.maximum(peak, by_shot[s])
    peak = 0.5 * jnp.max(peak, axis=0, keepdims=True) + 1.0
    factors = [(1.0 / math.sqrt(shots * groups)) / jnp.sqrt(by_shot[s] + peak) for s in range(shots)]
    def weigh(sources):
        notes = correct(sources) if sources else None
        for i in range(owned):
            for t in range(2 * tiles):
                total_t = None
                for s in range(shots):
                    part = factors[s][0:1] * spread[0, s, i, pl.ds(t * SUBLANES, SUBLANES)]
                    for g in range(1, groups):
                        part = part + factors[s][g:g + 1] * spread[g, s, i, pl.ds(t * SUBLANES, SUBLANES)]
                    total_t = part if total_t is None else total_t + part
                out_ref[i, pl.ds(t * SUBLANES, SUBLANES)] = total_t - notes[i][t] if notes else total_t

    def correct(sources):
        notes = [[zero] * (2 * tiles) for i in range(owned)]
        factor = factors[0]
        lane_row_shot = lax.rem(lax.broadcasted_iota(jnp.int32, (groups, LANES), 1) // (2 * tiles), shots)
        for s in range(1, shots):
            factor = jnp.where(lane_row_shot == s, factors[s], factor)
        origin = 2 * lax.rem(group * per_owner, per_pack) + 1
        for h in range(2):
            halo = zero
            for g in sources:
                halo = halo + factor[g:g + 1] * halves[g, h]
            for i in range(owned):
                for t in range(tiles):
                    value = None
                    for s in range(shots):
                        shift = 2 * LANES - origin - 2 * ((i * shots + s) * tiles + t)
                        moved = pltpu.roll(halo, shift, 1)
                        value = moved if value is None else value + moved
                    notes[i][h * tiles + t] = jnp.where(ends, value, 0.0)
        return notes

    noted = [(group < early, range(groups))] + [(late & (group == target), sources) for sources, target in pairs]
    plain = jnp.logical_not(noted[0][0] | noted[1][0] | noted[2][0])
    for here, sources in noted + [(plain, None)]:
        @pl.when(here)
        def _():
            weigh(sources)

    pltpu.make_async_copy(inbox.at[pl.ds(0, devices - 1)], inbox.at[pl.ds(0, devices - 1)], note_send).wait()
    for g in range(early):
        for extra in (False, True):
            sent = min(g + 1, early) + extra

            @pl.when(((group == g + 1) if g + 1 < early else (group > g)) & (any_ahead == extra))
            def _():
                pltpu.make_async_copy(halo_in.at[pl.ds(0, sent)], halo_in.at[pl.ds(0, sent)], edge_send).wait()

    others = send.at[pl.ds(0, groups - 1)]
    pltpu.make_async_copy(others, others, bulk_send).wait()


def on_device(correlation, illumination, aperture):
    shots, rows, cols, slab = correlation.shape
    groups = lax.axis_size("shot")
    slabs = lax.axis_size("depth")
    owned = rows // groups
    half = cols // 2
    tiles = half // SUBLANES
    dims = (shots, rows, cols, slab, groups, slabs, owned, rows * cols * slab * slabs)
    packs = -(-rows * shots * tiles // (LANES // 2))
    block = (shots * owned * (half + 2) + shots, slab)
    f32 = jnp.float32
    dma = pltpu.SemaphoreType.DMA
    regular = pltpu.SemaphoreType.REGULAR
    return pl.pallas_call(
        functools.partial(kernel, dims),
        out_shape=pltpu.VMEM((owned, cols, slab), f32),
        in_specs=[pl.BlockSpec(memory_space=pl.ANY)] * 3,
        out_specs=pl.BlockSpec(memory_space=pltpu.VMEM),
        scratch_shapes=[
            pltpu.SMEM(aperture.shape, jnp.int32),
            pltpu.VMEM((2, shots, rows, cols, slab), f32),
            pltpu.VMEM((shots, rows + 2, half + 2 * SUBLANES, slab), f32),
            pltpu.VMEM((shots, rows, half, slab), f32),
            pltpu.VMEM((packs, SUBLANES, LANES), f32),
            pltpu.VMEM((2, packs, SUBLANES, LANES), f32),
            pltpu.VMEM((packs, SUBLANES, LANES), f32),
            pltpu.VMEM((groups, SUBLANES, LANES), f32),
            pltpu.VMEM((groups, 2, SUBLANES, LANES), f32),
            pltpu.VMEM(block, f32),
            pltpu.VMEM((groups,) + block, f32),
            pltpu.VMEM((groups,) + block, f32),
            pltpu.VMEM((SUBLANES, LANES), f32),
            pltpu.VMEM((slabs * groups, LANES), f32),
            pltpu.VMEM((groups, shots, owned, cols, slab), f32),
            regular((groups - 1,)),
            regular,
            dma,
            dma,
            dma,
            dma((groups // 2,)),
            dma,
            dma,
            dma,
        ],
        compiler_params=pltpu.CompilerParams(collective_id=0, has_side_effects=True),
    )(correlation, illumination, aperture)


def solution(mesh):
    return jax.shard_map(
        on_device,
        mesh=mesh,
        in_specs=(P("shot", None, None, "depth"), P("shot", None, None, "depth"), P("shot", None)),
        out_specs=P("shot", None, "depth"),
        check_vma=False,
    )
```

```python
import functools
import math

import jax
import jax.numpy as jnp
from jax import lax
from jax.experimental import pallas as pl
from jax.experimental.pallas import tpu as pltpu
from jax.sharding import PartitionSpec as P

MESH = pl.DeviceIdType.MESH
LANES = 128
SUBLANES = 8
EARLY = 1


def kernel(dims, corr_hbm, ill_hbm, box_hbm, out_ref, box, raw, norm, centre, edge_out, edge_in, halo_out, halo_in, halves, spare, send, recv, message, inbox, spread,
           ready, passed, edge_send, edge_recv, bulk_send, bulk_recv, halo_recv, note_send, note_recv):
    shots, rows, cols, slab, groups, slabs, owned, cells = dims
    half = cols // 2
    tiles = half // SUBLANES
    devices = groups * slabs
    per_pack = LANES // 2
    per_owner = owned * shots * tiles
    group = lax.axis_index("shot")
    depth = lax.axis_index("depth")
    border = shots * owned * half
    placed = border + 2 * shots * owned
    corr, ill = raw.at[0], raw.at[1]

    box_copy = pltpu.make_async_copy(box_hbm, box, bulk_send)
    box_copy.start()
    for s in range(shots):
        for source, target in ((corr_hbm, corr), (ill_hbm, ill)):
            pltpu.make_async_copy(source.at[s], target.at[s], (note_send, edge_send)[s % 2]).start()

    def signal(semaphore, **device):
        pl.semaphore_signal(semaphore, inc=1, device_id=device, device_id_type=MESH)

    def each(low, high, action):
        lax.fori_loop(low, high, lambda t, carry: (action(t), carry)[1], 0)

    barrier = pltpu.get_barrier_semaphore()
    each(1, slabs, lambda d: signal(barrier, depth=lax.rem(depth + d, slabs)))
    each(group + 1, groups, lambda g: signal(barrier, shot=g))

    lane = lax.broadcasted_iota(jnp.int32, (SUBLANES, LANES), 1)
    sub = lax.broadcasted_iota(jnp.int32, (SUBLANES, LANES), 0)
    zero = jnp.zeros((SUBLANES, slab), jnp.float32)
    for s in range(shots):
        for r in (0, rows + 1):
            for t in range(tiles + 2):
                norm[s, r, pl.ds(t * SUBLANES, SUBLANES)] = zero
    packs = edge_out.shape[0]

    @pl.when(depth == 0)
    def _():
        for p in range(packs):
            edge_in[0, p] = zero

    @pl.when(depth == slabs - 1)
    def _():
        for p in range(packs):
            edge_in[1, p] = zero

    box_copy.wait()
    lower = []
    upper = []
    start = []
    for s in range(shots):
        first, last = box[s, 2], box[s, 3]
        start.append(jnp.minimum(first, half))
        lower.append([(sub + t * SUBLANES >= first) & (sub + t * SUBLANES < last) for t in range(tiles)])
        upper.append([(sub + t * SUBLANES + half >= first) & (sub + t * SUBLANES + half < last) for t in range(tiles)])

    def lane_of(r, s, t):
        k = (r * shots + s) * tiles + t
        return k // per_pack, 2 * (k % per_pack)

    packed = [zero] * packs
    for s in range(shots):
        if s < 2:
            pair = raw.at[:, pl.ds(0, len(range(s, shots, 2)))]
            pltpu.make_async_copy(pair, pair, (note_send, edge_send)[s]).wait()
        for r in range(rows):
            in_row = (r >= box[s, 0]) & (r < box[s, 1])
            parts = []
            for t in range(tiles):
                here = pl.ds(t * SUBLANES, SUBLANES)
                there = pl.ds(t * SUBLANES + half, SUBLANES)
                top = jnp.where(upper[s][t], corr[s, r, there], corr[s, r, here])
                top = jnp.where((lower[s][t] | upper[s][t]) & in_row, top, 0.0)
                value = top / (jnp.where(upper[s][t], ill[s, r, there], ill[s, r, here]) + 0.1)
                parts.append(value)
                p, k = lane_of(r, s, t)
                packed[p] = jnp.where(lane // 2 == k // 2, pltpu.roll(value, k + 1, 1), packed[p])
            for t, value in enumerate([parts[-1]] + parts + [parts[0]]):
                norm[s, r + 1, pl.ds(t * SUBLANES, SUBLANES)] = value
    for p in range(packs):
        edge_out[p] = packed[p]

    def edge_copy(side):
        return pltpu.make_async_remote_copy(
            src_ref=edge_out, dst_ref=edge_in.at[1 - side], send_sem=edge_send,
            recv_sem=edge_recv, device_id={"depth": depth + (1 if side else -1)}, device_id_type=MESH)

    def laplacian():
        row_index = lax.broadcasted_iota(jnp.int32, (rows, slab), 0)
        energies = []
        for s in range(shots):
            in_rows = (row_index >= box[s, 0]) & (row_index < box[s, 1])
            energy = None
            for side, column in enumerate((start[s], start[s] + half - 1)):
                in_box = (column >= box[s, 2]) & (column < box[s, 3])
                value = jnp.where(in_rows & in_box, corr[s, :, column], 0.0) / (ill[s, :, column] + 0.1)
                for owner in range(groups):
                    send[owner, pl.ds(border + (2 * s + side) * owned, owned)] = 0.0 - value[owner * owned:(owner + 1) * owned]
                in_grid = (start[s] > 0) if side == 0 else (start[s] < cols - half)
                kept = jnp.where(in_grid, value, 0.0)
                kept = kept * kept
                energy = kept if energy is None else energy + kept
            while energy.shape[0] > SUBLANES:
                energy = energy[:energy.shape[0] // 2] + energy[energy.shape[0] // 2:]
            energies.append(energy)
            for owner in range(groups):
                send[owner, pl.ds(placed + s, 1)] = jnp.full((1, LANES), start[s].astype(jnp.float32))

        for r in range(rows):
            for s in range(shots):
                for t in range(tiles):
                    value = norm[s, r + 1, pl.ds((t + 1) * SUBLANES, SUBLANES)]
                    beside = jnp.where(lane > 0, pltpu.roll(value, 1, 1), 0.0)
                    beside = beside + jnp.where(lane < LANES - 1, pltpu.roll(value, LANES - 1, 1), 0.0)
                    centre[s, r, pl.ds(t * SUBLANES, SUBLANES)] = 6.0 * value - beside

        no_before = [[sub + t * SUBLANES == lax.rem(start[s], half) for t in range(tiles)] for s in range(shots)]
        no_after = [[sub + t * SUBLANES == lax.rem(start[s] + half - 1, half) for t in range(tiles)] for s in range(shots)]
        packed = [zero] * packs
        for r in range(rows):
            owner, i = r // owned, r % owned
            for s in range(shots):
                for t in range(tiles):
                    base = SUBLANES + t * SUBLANES
                    beside = norm[s, r, pl.ds(base, SUBLANES)] + norm[s, r + 2, pl.ds(base, SUBLANES)]
                    beside = beside + jnp.where(no_before[s][t], 0.0, norm[s, r + 1, pl.ds(base - 1, SUBLANES)])
                    beside = beside + jnp.where(no_after[s][t], 0.0, norm[s, r + 1, pl.ds(base + 1, SUBLANES)])
                    p, k = lane_of(r, s, t)
                    result = centre[s, r, pl.ds(t * SUBLANES, SUBLANES)] - beside
                    energies[s] = energies[s] + result * result
                    packed[p] = jnp.where(lane // 2 == k // 2, pltpu.roll(result, k + 1, 1), packed[p])
                    send[owner, pl.ds((s * owned + i) * half + t * SUBLANES, SUBLANES)] = result
        return tuple(energies) + tuple(packed)

    late = (lax.rem(depth, 2) == 1) & (depth < slabs - 1)
    before = lax.cond(late, laplacian, lambda: (zero,) * (shots + packs))

    pl.semaphore_wait(barrier, group + slabs - 1)

    @pl.when(depth > 0)
    def _():
        edge_copy(0).start()

    @pl.when(depth < slabs - 1)
    def _():
        edge_copy(1).start()

    each(0, group, lambda g: signal(ready.at[group - 1], shot=g))
    each(1, slabs, lambda d: signal(passed, depth=lax.rem(depth + d, slabs)))

    after = lax.cond(late, lambda: before, laplacian)
    energies, packed = list(after[:shots]), list(after[shots:])

    def bulk(g, origin):
        return pltpu.make_async_remote_copy(
            src_ref=send.at[g], dst_ref=recv.at[origin], send_sem=bulk_send, recv_sem=bulk_recv.at[lax.div(origin, 2)],
            device_id={"shot": g}, device_id_type=MESH)

    def halo_copy(g):
        return pltpu.make_async_remote_copy(
            src_ref=halo_out.at[g * per_owner // per_pack], dst_ref=halo_in.at[group], send_sem=edge_send,
            recv_sem=halo_recv, device_id={"shot": g}, device_id_type=MESH)

    early = min(EARLY, groups)
    quarter = groups // 4
    pairs = ((range(quarter, 2 * quarter), 2 * quarter), (range(2 * quarter, 3 * quarter), quarter))
    ahead = [late & (group >= sources[0]) & (group <= sources[-1]) for sources, target in pairs]
    for here, (sources, target) in zip(ahead, pairs):
        @pl.when(here)
        def _():
            spare[...] = send[target]

    for g in range(early):
        @pl.when(g < group)
        def _():
            bulk(g, group).start()

    any_ahead = ahead[0] | ahead[1]
    for here, (sources, target) in zip(ahead, pairs):
        @pl.when(here)
        def _():
            if target > sources[0]:
                pl.semaphore_wait(ready.at[target - 1], 1)
            pltpu.make_async_remote_copy(
                src_ref=spare, dst_ref=recv.at[group], send_sem=bulk_send, recv_sem=bulk_recv.at[lax.div(group, 2)],
                device_id={"shot": target}, device_id_type=MESH).start()

    for inner, count in ((True, 2), (False, 1)):
        @pl.when(((depth > 0) & (depth < slabs - 1)) == inner)
        def _():
            tile = edge_in.at[pl.ds(0, count)]
            pltpu.make_async_copy(tile, tile, edge_send).wait()
            pltpu.make_async_copy(tile, tile, edge_recv).wait()

    lane_shot = lax.rem(lane // (2 * tiles), shots)
    halos = []
    for p in range(packs):
        halo = jnp.where(lane % 2 == 0, pltpu.roll(edge_in[1, p], LANES - 1, 1), pltpu.roll(edge_in[0, p], 1, 1))
        halo_out[p] = halo
        halos.append(halo)
        change = halo * (halo - 2.0 * packed[p])
        for s in range(shots):
            energies[s] = energies[s] + jnp.where(lane_shot == s, change, 0.0)

    ends = (lane == 0) | (lane == LANES - 1)
    for owner in range(early, groups):
        for i in range(owned):
            for s in range(shots):
                for t in range(tiles):
                    p, k = lane_of(owner * owned + i, s, t)
                    here = pl.ds((s * owned + i) * half + t * SUBLANES, SUBLANES)
                    moved = pltpu.roll(halos[p], LANES - 1 - k, 1)
                    send[owner, here] = send[owner, here] - jnp.where(ends, moved, 0.0)

    def total(value):
        return jnp.sum(jnp.sum(value, axis=0, keepdims=True), axis=1, keepdims=True)

    note = jnp.zeros((1, LANES), jnp.float32)
    gap = LANES // shots
    lane_row = lax.broadcasted_iota(jnp.int32, (1, LANES), 1)
    for s in range(shots):
        note = jnp.where(lane_row // gap == s, total(energies[s]), note)
    message[pl.ds(0, 1)] = note / cells

    slot = depth * groups + group
    own_note = pltpu.make_async_copy(message.at[pl.ds(0, 1)], inbox.at[pl.ds(slot, 1)], note_recv)
    own_note.start()

    def tell(g, d):
        pltpu.make_async_remote_copy(
            src_ref=message.at[pl.ds(0, 1)], dst_ref=inbox.at[pl.ds(slot, 1)], send_sem=note_send, recv_sem=note_recv,
            device_id={"shot": g, "depth": d}, device_id_type=MESH).start()

    @pl.when((group > early) & (depth == 0))
    def _():
        bulk(early, group).start()

    pl.semaphore_wait(passed, slabs - 1)
    for g in range(groups):
        @pl.when(g < group)
        def _():
            for d in range(slabs):
                tell(g, d)
    for d in range(slabs):
        @pl.when(d != depth)
        def _():
            tell(group, d)
    for g in range(early):
        @pl.when(g < group)
        def _():
            halo_copy(g).start()

    for here, (sources, target) in zip(ahead, pairs):
        @pl.when(here)
        def _():
            halo_copy(target).start()

    for g in range(early, groups):
        @pl.when((g < group) & jnp.logical_not((ahead[1] & (g == pairs[1][1])) | ((depth == 0) & (g == early))))
        def _():
            bulk(g, group).start()
    for g in sorted(range(1, groups), key=lambda g: (g % 2, g) if 2 * g >= groups else (2, g)):
        @pl.when(g > group)
        def _():
            if g == pairs[0][1]:
                @pl.when(jnp.logical_not(ahead[0]))
                def _():
                    pl.semaphore_wait(ready.at[g - 1], 1)
                    bulk(g, group).start()
            else:
                pl.semaphore_wait(ready.at[g - 1], 1)
                bulk(g, group).start()
            for d in range(slabs):
                tell(g, d)

    recv[group] = send[group]

    col = [(sub + t * SUBLANES).astype(jnp.float32) for t in range(2 * tiles)]
    for g in range(groups):
        if g % 2 == 0:
            for own, count in ((True, 1), (False, 2)):
                @pl.when((lax.div(group, 2) == g // 2) == own)
                def _():
                    pair = recv.at[pl.ds(g, count)]
                    pltpu.make_async_copy(pair, pair, bulk_recv.at[g // 2]).wait()

        for s in range(shots):
            first = recv[g, pl.ds(placed + s, 1)]
            masks = []
            for t in range(2 * tiles):
                offset = col[t] - first
                masks.append((offset == -1.0, offset == float(half), (offset >= -1.0) & (offset <= float(half))))
            for i in range(owned):
                index = s * owned + i
                low = recv[g, pl.ds(border + 2 * s * owned + i, 1)]
                high = recv[g, pl.ds(border + (2 * s + 1) * owned + i, 1)]
                for t in range(2 * tiles):
                    at_low, at_high, inside = masks[t]
                    value = recv[g, pl.ds(index * half + (t % tiles) * SUBLANES, SUBLANES)]
                    value = jnp.where(at_low, low, jnp.where(at_high, high, value))
                    spread[g, s, i, pl.ds(t * SUBLANES, SUBLANES)] = jnp.where(inside, value, 0.0)

    def collect(sources, count):
        arrived = halo_in.at[pl.ds(0, count)]
        pltpu.make_async_copy(arrived, arrived, halo_recv).wait()
        fold_col = (lax.rem(lane // 2, tiles) * SUBLANES + sub).astype(jnp.float32)
        for g in sources:
            first = recv[g, pl.ds(placed, 1)]
            for s in range(1, shots):
                first = jnp.where(lane_shot == s, recv[g, pl.ds(placed + s, 1)], first)
            halo = halo_in[g]
            halves[g, 0] = jnp.where(fold_col >= first, halo, 0.0)
            halves[g, 1] = jnp.where(fold_col >= first, 0.0, halo)

    @pl.when(group < early)
    def _():
        halo_in[group] = halo_out[lax.div(group * per_owner, per_pack)]
        collect(range(groups), groups - 1)

    for sources, target in pairs:
        @pl.when(late & (group == target))
        def _():
            collect(sources, len(sources))

    pltpu.make_async_copy(inbox, inbox, note_recv).wait()
    meansq = inbox[pl.ds(0, groups)]
    for d in range(1, slabs):
        meansq = meansq + inbox[pl.ds(d * groups, groups)]
    lane_group = lax.broadcasted_iota(jnp.int32, (groups, LANES), 1) // gap
    turned = [meansq] + [pltpu.roll(meansq, j * gap, 1) for j in range(1, shots)]
    by_shot = []
    for s in range(shots):
        value = meansq
        for j in range(1, shots):
            value = jnp.where(lane_group == (s + j) % shots, turned[j], value)
        by_shot.append(value)
    peak = by_shot[0]
    for s in range(1, shots):
        peak = jnp.maximum(peak, by_shot[s])
    peak = 0.5 * jnp.max(peak, axis=0, keepdims=True) + 1.0
    factors = [(1.0 / math.sqrt(shots * groups)) / jnp.sqrt(by_shot[s] + peak) for s in range(shots)]
    def weigh(sources):
        notes = correct(sources) if sources else None
        for i in range(owned):
            for t in range(2 * tiles):
                total_t = None
                for s in range(shots):
                    part = factors[s][0:1] * spread[0, s, i, pl.ds(t * SUBLANES, SUBLANES)]
                    for g in range(1, groups):
                        part = part + factors[s][g:g + 1] * spread[g, s, i, pl.ds(t * SUBLANES, SUBLANES)]
                    total_t = part if total_t is None else total_t + part
                out_ref[i, pl.ds(t * SUBLANES, SUBLANES)] = total_t - notes[i][t] if notes else total_t

    def correct(sources):
        notes = [[zero] * (2 * tiles) for i in range(owned)]
        factor = factors[0]
        lane_row_shot = lax.rem(lax.broadcasted_iota(jnp.int32, (groups, LANES), 1) // (2 * tiles), shots)
        for s in range(1, shots):
            factor = jnp.where(lane_row_shot == s, factors[s], factor)
        origin = 2 * lax.rem(group * per_owner, per_pack) + 1
        for h in range(2):
            halo = zero
            for g in sources:
                halo = halo + factor[g:g + 1] * halves[g, h]
            for i in range(owned):
                for t in range(tiles):
                    value = None
                    for s in range(shots):
                        shift = 2 * LANES - origin - 2 * ((i * shots + s) * tiles + t)
                        moved = pltpu.roll(halo, shift, 1)
                        value = moved if value is None else value + moved
                    notes[i][h * tiles + t] = jnp.where(ends, value, 0.0)
        return notes

    noted = [(group < early, range(groups))] + [(late & (group == target), sources) for sources, target in pairs]
    plain = jnp.logical_not(noted[0][0] | noted[1][0] | noted[2][0])
    for here, sources in noted + [(plain, None)]:
        @pl.when(here)
        def _():
            weigh(sources)

    pltpu.make_async_copy(inbox.at[pl.ds(0, devices - 1)], inbox.at[pl.ds(0, devices - 1)], note_send).wait()
    for g in range(early):
        for extra in (False, True):
            sent = min(g + 1, early) + extra

            @pl.when(((group == g + 1) if g + 1 < early else (group > g)) & (any_ahead == extra))
            def _():
                pltpu.make_async_copy(halo_in.at[pl.ds(0, sent)], halo_in.at[pl.ds(0, sent)], edge_send).wait()

    others = send.at[pl.ds(0, groups - 1)]
    pltpu.make_async_copy(others, others, bulk_send).wait()


def on_device(correlation, illumination, aperture):
    shots, rows, cols, slab = correlation.shape
    groups = lax.axis_size("shot")
    slabs = lax.axis_size("depth")
    owned = rows // groups
    half = cols // 2
    tiles = half // SUBLANES
    dims = (shots, rows, cols, slab, groups, slabs, owned, rows * cols * slab * slabs)
    packs = -(-rows * shots * tiles // (LANES // 2))
    block = (shots * owned * (half + 2) + shots, slab)
    f32 = jnp.float32
    dma = pltpu.SemaphoreType.DMA
    regular = pltpu.SemaphoreType.REGULAR
    return pl.pallas_call(
        functools.partial(kernel, dims),
        out_shape=pltpu.VMEM((owned, cols, slab), f32),
        in_specs=[pl.BlockSpec(memory_space=pl.ANY)] * 3,
        out_specs=pl.BlockSpec(memory_space=pltpu.VMEM),
        scratch_shapes=[
            pltpu.SMEM(aperture.shape, jnp.int32),
            pltpu.VMEM((2, shots, rows, cols, slab), f32),
            pltpu.VMEM((shots, rows + 2, half + 2 * SUBLANES, slab), f32),
            pltpu.VMEM((shots, rows, half, slab), f32),
            pltpu.VMEM((packs, SUBLANES, LANES), f32),
            pltpu.VMEM((2, packs, SUBLANES, LANES), f32),
            pltpu.VMEM((packs, SUBLANES, LANES), f32),
            pltpu.VMEM((groups, SUBLANES, LANES), f32),
            pltpu.VMEM((groups, 2, SUBLANES, LANES), f32),
            pltpu.VMEM(block, f32),
            pltpu.VMEM((groups,) + block, f32),
            pltpu.VMEM((groups,) + block, f32),
            pltpu.VMEM((SUBLANES, LANES), f32),
            pltpu.VMEM((slabs * groups, LANES), f32),
            pltpu.VMEM((groups, shots, owned, cols, slab), f32),
            regular((groups - 1,)),
            regular,
            dma,
            dma,
            dma,
            dma((groups // 2,)),
            dma,
            dma,
            dma,
        ],
        compiler_params=pltpu.CompilerParams(collective_id=0, has_side_effects=True),
    )(correlation, illumination, aperture)


def solution(mesh):
    return jax.shard_map(
        on_device,
        mesh=mesh,
        in_specs=(P("shot", None, None, "depth"), P("shot", None, None, "depth"), P("shot", None)),
        out_specs=P("shot", None, "depth"),
        check_vma=False,
    )
```

```python
import functools
import math

import jax
import jax.numpy as jnp
from jax import lax
from jax.experimental import pallas as pl
from jax.experimental.pallas import tpu as pltpu
from jax.sharding import PartitionSpec as P

MESH = pl.DeviceIdType.MESH
LANES = 128
SUBLANES = 8
EARLY = 1


def kernel(dims, corr_hbm, ill_hbm, box_hbm, out_ref, box, raw, norm, centre, edge_out, edge_in, halo_out, halo_in, halves, spare, send, recv, message, inbox, spread,
           ready, passed, edge_send, edge_recv, bulk_send, bulk_recv, halo_recv, note_send, note_recv):
    shots, rows, cols, slab, groups, slabs, owned, cells = dims
    half = cols // 2
    tiles = half // SUBLANES
    devices = groups * slabs
    per_pack = LANES // 2
    per_owner = owned * shots * tiles
    group = lax.axis_index("shot")
    depth = lax.axis_index("depth")
    border = shots * owned * half
    placed = border + 2 * shots * owned
    corr, ill = raw.at[0], raw.at[1]

    box_copy = pltpu.make_async_copy(box_hbm, box, bulk_send)
    box_copy.start()
    for s in range(shots):
        for source, target in ((corr_hbm, corr), (ill_hbm, ill)):
            pltpu.make_async_copy(source.at[s], target.at[s], (note_send, edge_send)[s % 2]).start()

    def signal(semaphore, **device):
        pl.semaphore_signal(semaphore, inc=1, device_id=device, device_id_type=MESH)

    def each(low, high, action):
        lax.fori_loop(low, high, lambda t, carry: (action(t), carry)[1], 0)

    barrier = pltpu.get_barrier_semaphore()
    each(1, slabs, lambda d: signal(barrier, depth=lax.rem(depth + d, slabs)))
    each(group + 1, groups, lambda g: signal(barrier, shot=g))

    lane = lax.broadcasted_iota(jnp.int32, (SUBLANES, LANES), 1)
    sub = lax.broadcasted_iota(jnp.int32, (SUBLANES, LANES), 0)
    zero = jnp.zeros((SUBLANES, slab), jnp.float32)
    for s in range(shots):
        for r in (0, rows + 1):
            for t in range(tiles + 2):
                norm[s, r, pl.ds(t * SUBLANES, SUBLANES)] = zero
    packs = edge_out.shape[0]

    @pl.when(depth == 0)
    def _():
        for p in range(packs):
            edge_in[0, p] = zero

    @pl.when(depth == slabs - 1)
    def _():
        for p in range(packs):
            edge_in[1, p] = zero

    box_copy.wait()
    lower = []
    upper = []
    start = []
    for s in range(shots):
        first, last = box[s, 2], box[s, 3]
        start.append(jnp.minimum(first, half))
        lower.append([(sub + t * SUBLANES >= first) & (sub + t * SUBLANES < last) for t in range(tiles)])
        upper.append([(sub + t * SUBLANES + half >= first) & (sub + t * SUBLANES + half < last) for t in range(tiles)])

    def lane_of(r, s, t):
        k = (r * shots + s) * tiles + t
        return k // per_pack, 2 * (k % per_pack)

    packed = [zero] * packs
    for s in range(shots):
        if s < 2:
            pair = raw.at[:, pl.ds(0, len(range(s, shots, 2)))]
            pltpu.make_async_copy(pair, pair, (note_send, edge_send)[s]).wait()
        for r in range(rows):
            in_row = (r >= box[s, 0]) & (r < box[s, 1])
            parts = []
            for t in range(tiles):
                here = pl.ds(t * SUBLANES, SUBLANES)
                there = pl.ds(t * SUBLANES + half, SUBLANES)
                top = jnp.where(upper[s][t], corr[s, r, there], corr[s, r, here])
                top = jnp.where((lower[s][t] | upper[s][t]) & in_row, top, 0.0)
                value = top / (jnp.where(upper[s][t], ill[s, r, there], ill[s, r, here]) + 0.1)
                parts.append(value)
                p, k = lane_of(r, s, t)
                packed[p] = jnp.where(lane // 2 == k // 2, pltpu.roll(value, k + 1, 1), packed[p])
            for t, value in enumerate([parts[-1]] + parts + [parts[0]]):
                norm[s, r + 1, pl.ds(t * SUBLANES, SUBLANES)] = value
    for p in range(packs):
        edge_out[p] = packed[p]

    def edge_copy(side):
        return pltpu.make_async_remote_copy(
            src_ref=edge_out, dst_ref=edge_in.at[1 - side], send_sem=edge_send,
            recv_sem=edge_recv, device_id={"depth": depth + (1 if side else -1)}, device_id_type=MESH)

    def laplacian():
        row_index = lax.broadcasted_iota(jnp.int32, (rows, slab), 0)
        energies = []
        for s in range(shots):
            in_rows = (row_index >= box[s, 0]) & (row_index < box[s, 1])
            energy = None
            for side, column in enumerate((start[s], start[s] + half - 1)):
                in_box = (column >= box[s, 2]) & (column < box[s, 3])
                value = jnp.where(in_rows & in_box, corr[s, :, column], 0.0) / (ill[s, :, column] + 0.1)
                for owner in range(groups):
                    send[owner, pl.ds(border + (2 * s + side) * owned, owned)] = 0.0 - value[owner * owned:(owner + 1) * owned]
                in_grid = (start[s] > 0) if side == 0 else (start[s] < cols - half)
                kept = jnp.where(in_grid, value, 0.0)
                kept = kept * kept
                energy = kept if energy is None else energy + kept
            while energy.shape[0] > SUBLANES:
                energy = energy[:energy.shape[0] // 2] + energy[energy.shape[0] // 2:]
            energies.append(energy)
            for owner in range(groups):
                send[owner, pl.ds(placed + s, 1)] = jnp.full((1, LANES), start[s].astype(jnp.float32))

        for r in range(rows):
            for s in range(shots):
                for t in range(tiles):
                    value = norm[s, r + 1, pl.ds((t + 1) * SUBLANES, SUBLANES)]
                    beside = jnp.where(lane > 0, pltpu.roll(value, 1, 1), 0.0)
                    beside = beside + jnp.where(lane < LANES - 1, pltpu.roll(value, LANES - 1, 1), 0.0)
                    centre[s, r, pl.ds(t * SUBLANES, SUBLANES)] = 6.0 * value - beside

        no_before = [[sub + t * SUBLANES == lax.rem(start[s], half) for t in range(tiles)] for s in range(shots)]
        no_after = [[sub + t * SUBLANES == lax.rem(start[s] + half - 1, half) for t in range(tiles)] for s in range(shots)]
        packed = [zero] * packs
        for r in range(rows):
            owner, i = r // owned, r % owned
            for s in range(shots):
                for t in range(tiles):
                    base = SUBLANES + t * SUBLANES
                    beside = norm[s, r, pl.ds(base, SUBLANES)] + norm[s, r + 2, pl.ds(base, SUBLANES)]
                    beside = beside + jnp.where(no_before[s][t], 0.0, norm[s, r + 1, pl.ds(base - 1, SUBLANES)])
                    beside = beside + jnp.where(no_after[s][t], 0.0, norm[s, r + 1, pl.ds(base + 1, SUBLANES)])
                    p, k = lane_of(r, s, t)
                    result = centre[s, r, pl.ds(t * SUBLANES, SUBLANES)] - beside
                    energies[s] = energies[s] + result * result
                    packed[p] = jnp.where(lane // 2 == k // 2, pltpu.roll(result, k + 1, 1), packed[p])
                    send[owner, pl.ds((s * owned + i) * half + t * SUBLANES, SUBLANES)] = result
        return tuple(energies) + tuple(packed)

    late = (lax.rem(depth, 2) == 1) & (depth < slabs - 1)
    before = lax.cond(late, laplacian, lambda: (zero,) * (shots + packs))

    pl.semaphore_wait(barrier, group + slabs - 1)

    @pl.when(depth > 0)
    def _():
        edge_copy(0).start()

    @pl.when(depth < slabs - 1)
    def _():
        edge_copy(1).start()

    each(0, group, lambda g: signal(ready.at[group - 1], shot=g))
    each(1, slabs, lambda d: signal(passed, depth=lax.rem(depth + d, slabs)))

    after = lax.cond(late, lambda: before, laplacian)
    energies, packed = list(after[:shots]), list(after[shots:])

    def bulk(g, origin):
        return pltpu.make_async_remote_copy(
            src_ref=send.at[g], dst_ref=recv.at[origin], send_sem=bulk_send, recv_sem=bulk_recv.at[lax.div(origin, 2)],
            device_id={"shot": g}, device_id_type=MESH)

    def halo_copy(g):
        return pltpu.make_async_remote_copy(
            src_ref=halo_out.at[g * per_owner // per_pack], dst_ref=halo_in.at[group], send_sem=edge_send,
            recv_sem=halo_recv, device_id={"shot": g}, device_id_type=MESH)

    early = min(EARLY, groups)
    quarter = groups // 4
    pairs = ((range(quarter, 2 * quarter), 2 * quarter), (range(2 * quarter, 3 * quarter), quarter))
    ahead = [late & (group >= sources[0]) & (group <= sources[-1]) for sources, target in pairs]
    for here, (sources, target) in zip(ahead, pairs):
        @pl.when(here)
        def _():
            spare[...] = send[target]

    for g in range(early):
        @pl.when(g < group)
        def _():
            bulk(g, group).start()

    any_ahead = ahead[0] | ahead[1]
    for here, (sources, target) in zip(ahead, pairs):
        @pl.when(here)
        def _():
            if target > sources[0]:
                pl.semaphore_wait(ready.at[target - 1], 1)
            pltpu.make_async_remote_copy(
                src_ref=spare, dst_ref=recv.at[group], send_sem=bulk_send, recv_sem=bulk_recv.at[lax.div(group, 2)],
                device_id={"shot": target}, device_id_type=MESH).start()

    for inner, count in ((True, 2), (False, 1)):
        @pl.when(((depth > 0) & (depth < slabs - 1)) == inner)
        def _():
            tile = edge_in.at[pl.ds(0, count)]
            pltpu.make_async_copy(tile, tile, edge_send).wait()
            pltpu.make_async_copy(tile, tile, edge_recv).wait()

    lane_shot = lax.rem(lane // (2 * tiles), shots)
    halos = []
    for p in range(packs):
        halo = jnp.where(lane % 2 == 0, pltpu.roll(edge_in[1, p], LANES - 1, 1), pltpu.roll(edge_in[0, p], 1, 1))
        halo_out[p] = halo
        halos.append(halo)
        change = halo * (halo - 2.0 * packed[p])
        for s in range(shots):
            energies[s] = energies[s] + jnp.where(lane_shot == s, change, 0.0)

    ends = (lane == 0) | (lane == LANES - 1)
    for owner in range(early, groups):
        for i in range(owned):
            for s in range(shots):
                for t in range(tiles):
                    p, k = lane_of(owner * owned + i, s, t)
                    here = pl.ds((s * owned + i) * half + t * SUBLANES, SUBLANES)
                    moved = pltpu.roll(halos[p], LANES - 1 - k, 1)
                    send[owner, here] = send[owner, here] - jnp.where(ends, moved, 0.0)

    def total(value):
        return jnp.sum(jnp.sum(value, axis=0, keepdims=True), axis=1, keepdims=True)

    note = jnp.zeros((1, LANES), jnp.float32)
    gap = LANES // shots
    lane_row = lax.broadcasted_iota(jnp.int32, (1, LANES), 1)
    for s in range(shots):
        note = jnp.where(lane_row // gap == s, total(energies[s]), note)
    message[pl.ds(0, 1)] = note / cells

    slot = depth * groups + group
    own_note = pltpu.make_async_copy(message.at[pl.ds(0, 1)], inbox.at[pl.ds(slot, 1)], note_recv)
    own_note.start()

    def tell(g, d):
        pltpu.make_async_remote_copy(
            src_ref=message.at[pl.ds(0, 1)], dst_ref=inbox.at[pl.ds(slot, 1)], send_sem=note_send, recv_sem=note_recv,
            device_id={"shot": g, "depth": d}, device_id_type=MESH).start()

    @pl.when((group > early) & (depth == 0))
    def _():
        bulk(early, group).start()

    pl.semaphore_wait(passed, slabs - 1)
    for g in range(groups):
        @pl.when(g < group)
        def _():
            for d in range(slabs):
                tell(g, d)
    for d in range(slabs):
        @pl.when(d != depth)
        def _():
            tell(group, d)
    for g in range(early):
        @pl.when(g < group)
        def _():
            halo_copy(g).start()

    for here, (sources, target) in zip(ahead, pairs):
        @pl.when(here)
        def _():
            halo_copy(target).start()

    for g in range(early, groups):
        @pl.when((g < group) & jnp.logical_not((ahead[1] & (g == pairs[1][1])) | ((depth == 0) & (g == early))))
        def _():
            bulk(g, group).start()
    for g in sorted(range(1, groups), key=lambda g: (g % 2, g) if 2 * g >= groups else (2, g)):
        @pl.when(g > group)
        def _():
            if g == pairs[0][1]:
                @pl.when(jnp.logical_not(ahead[0]))
                def _():
                    pl.semaphore_wait(ready.at[g - 1], 1)
                    bulk(g, group).start()
            else:
                pl.semaphore_wait(ready.at[g - 1], 1)
                bulk(g, group).start()
            for d in range(slabs):
                tell(g, d)

    recv[group] = send[group]

    col = [(sub + t * SUBLANES).astype(jnp.float32) for t in range(2 * tiles)]
    for g in range(groups):
        if g % 2 == 0:
            for own, count in ((True, 1), (False, 2)):
                @pl.when((lax.div(group, 2) == g // 2) == own)
                def _():
                    pair = recv.at[pl.ds(g, count)]
                    pltpu.make_async_copy(pair, pair, bulk_recv.at[g // 2]).wait()

        for s in range(shots):
            first = recv[g, pl.ds(placed + s, 1)]
            masks = []
            for t in range(2 * tiles):
                offset = col[t] - first
                masks.append((offset == -1.0, offset == float(half), (offset >= -1.0) & (offset <= float(half))))
            for i in range(owned):
                index = s * owned + i
                low = recv[g, pl.ds(border + 2 * s * owned + i, 1)]
                high = recv[g, pl.ds(border + (2 * s + 1) * owned + i, 1)]
                for t in range(2 * tiles):
                    at_low, at_high, inside = masks[t]
                    value = recv[g, pl.ds(index * half + (t % tiles) * SUBLANES, SUBLANES)]
                    value = jnp.where(at_low, low, jnp.where(at_high, high, value))
                    spread[g, s, i, pl.ds(t * SUBLANES, SUBLANES)] = jnp.where(inside, value, 0.0)

    def collect(sources, count):
        arrived = halo_in.at[pl.ds(0, count)]
        pltpu.make_async_copy(arrived, arrived, halo_recv).wait()
        fold_col = (lax.rem(lane // 2, tiles) * SUBLANES + sub).astype(jnp.float32)
        for g in sources:
            first = recv[g, pl.ds(placed, 1)]
            for s in range(1, shots):
                first = jnp.where(lane_shot == s, recv[g, pl.ds(placed + s, 1)], first)
            halo = halo_in[g]
            halves[g, 0] = jnp.where(fold_col >= first, halo, 0.0)
            halves[g, 1] = jnp.where(fold_col >= first, 0.0, halo)

    @pl.when(group < early)
    def _():
        halo_in[group] = halo_out[lax.div(group * per_owner, per_pack)]
        collect(range(groups), groups - 1)

    for sources, target in pairs:
        @pl.when(late & (group == target))
        def _():
            collect(sources, len(sources))

    pltpu.make_async_copy(inbox.at[pl.ds(0, devices - 1)], inbox.at[pl.ds(0, devices - 1)], note_send).wait()
    for g in range(early):
        for extra in (False, True):
            sent = min(g + 1, early) + extra

            @pl.when(((group == g + 1) if g + 1 < early else (group > g)) & (any_ahead == extra))
            def _():
                pltpu.make_async_copy(halo_in.at[pl.ds(0, sent)], halo_in.at[pl.ds(0, sent)], edge_send).wait()

    others = send.at[pl.ds(0, groups - 1)]
    pltpu.make_async_copy(others, others, bulk_send).wait()

    pltpu.make_async_copy(inbox, inbox, note_recv).wait()
    meansq = inbox[pl.ds(0, groups)]
    for d in range(1, slabs):
        meansq = meansq + inbox[pl.ds(d * groups, groups)]
    lane_group = lax.broadcasted_iota(jnp.int32, (groups, LANES), 1) // gap
    turned = [meansq] + [pltpu.roll(meansq, j * gap, 1) for j in range(1, shots)]
    by_shot = []
    for s in range(shots):
        value = meansq
        for j in range(1, shots):
            value = jnp.where(lane_group == (s + j) % shots, turned[j], value)
        by_shot.append(value)
    peak = by_shot[0]
    for s in range(1, shots):
        peak = jnp.maximum(peak, by_shot[s])
    peak = 0.5 * jnp.max(peak, axis=0, keepdims=True) + 1.0
    factors = [(1.0 / math.sqrt(shots * groups)) / jnp.sqrt(by_shot[s] + peak) for s in range(shots)]
    def weigh(sources):
        notes = correct(sources) if sources else None
        for i in range(owned):
            for t in range(2 * tiles):
                total_t = None
                for s in range(shots):
                    part = factors[s][0:1] * spread[0, s, i, pl.ds(t * SUBLANES, SUBLANES)]
                    for g in range(1, groups):
                        part = part + factors[s][g:g + 1] * spread[g, s, i, pl.ds(t * SUBLANES, SUBLANES)]
                    total_t = part if total_t is None else total_t + part
                out_ref[i, pl.ds(t * SUBLANES, SUBLANES)] = total_t - notes[i][t] if notes else total_t

    def correct(sources):
        notes = [[zero] * (2 * tiles) for i in range(owned)]
        factor = factors[0]
        lane_row_shot = lax.rem(lax.broadcasted_iota(jnp.int32, (groups, LANES), 1) // (2 * tiles), shots)
        for s in range(1, shots):
            factor = jnp.where(lane_row_shot == s, factors[s], factor)
        origin = 2 * lax.rem(group * per_owner, per_pack) + 1
        for h in range(2):
            halo = zero
            for g in sources:
                halo = halo + factor[g:g + 1] * halves[g, h]
            for i in range(owned):
                for t in range(tiles):
                    value = None
                    for s in range(shots):
                        shift = 2 * LANES - origin - 2 * ((i * shots + s) * tiles + t)
                        moved = pltpu.roll(halo, shift, 1)
                        value = moved if value is None else value + moved
                    notes[i][h * tiles + t] = jnp.where(ends, value, 0.0)
        return notes

    noted = [(group < early, range(groups))] + [(late & (group == target), sources) for sources, target in pairs]
    plain = jnp.logical_not(noted[0][0] | noted[1][0] | noted[2][0])
    for here, sources in noted + [(plain, None)]:
        @pl.when(here)
        def _():
            weigh(sources)


def on_device(correlation, illumination, aperture):
    shots, rows, cols, slab = correlation.shape
    groups = lax.axis_size("shot")
    slabs = lax.axis_size("depth")
    owned = rows // groups
    half = cols // 2
    tiles = half // SUBLANES
    dims = (shots, rows, cols, slab, groups, slabs, owned, rows * cols * slab * slabs)
    packs = -(-rows * shots * tiles // (LANES // 2))
    block = (shots * owned * (half + 2) + shots, slab)
    f32 = jnp.float32
    dma = pltpu.SemaphoreType.DMA
    regular = pltpu.SemaphoreType.REGULAR
    return pl.pallas_call(
        functools.partial(kernel, dims),
        out_shape=pltpu.VMEM((owned, cols, slab), f32),
        in_specs=[pl.BlockSpec(memory_space=pl.ANY)] * 3,
        out_specs=pl.BlockSpec(memory_space=pltpu.VMEM),
        scratch_shapes=[
            pltpu.SMEM(aperture.shape, jnp.int32),
            pltpu.VMEM((2, shots, rows, cols, slab), f32),
            pltpu.VMEM((shots, rows + 2, half + 2 * SUBLANES, slab), f32),
            pltpu.VMEM((shots, rows, half, slab), f32),
            pltpu.VMEM((packs, SUBLANES, LANES), f32),
            pltpu.VMEM((2, packs, SUBLANES, LANES), f32),
            pltpu.VMEM((packs, SUBLANES, LANES), f32),
            pltpu.VMEM((groups, SUBLANES, LANES), f32),
            pltpu.VMEM((groups, 2, SUBLANES, LANES), f32),
            pltpu.VMEM(block, f32),
            pltpu.VMEM((groups,) + block, f32),
            pltpu.VMEM((groups,) + block, f32),
            pltpu.VMEM((SUBLANES, LANES), f32),
            pltpu.VMEM((slabs * groups, LANES), f32),
            pltpu.VMEM((groups, shots, owned, cols, slab), f32),
            regular((groups - 1,)),
            regular,
            dma,
            dma,
            dma,
            dma((groups // 2,)),
            dma,
            dma,
            dma,
        ],
        compiler_params=pltpu.CompilerParams(collective_id=0, has_side_effects=True),
    )(correlation, illumination, aperture)


def solution(mesh):
    return jax.shard_map(
        on_device,
        mesh=mesh,
        in_specs=(P("shot", None, None, "depth"), P("shot", None, None, "depth"), P("shot", None)),
        out_specs=P("shot", None, "depth"),
        check_vma=False,
    )
```
